256 devices in a mesh: comm: 8 (over z), arc: 32 (over y, x, core).
Axes of the slice: x: 4, y: 4, z: 8, core: 2. Of those that a mesh axis runs over, the one named last changes fastest.
Arguments:
- prev_dist: float32 [1024, 8192], P('comm', 'arc'), may hold values from 0 to 4
- source_node: int32 [1024], P('comm'), may hold values from 0 to 8191, as said below
- arc_tail: int32 [16, 8192], P(None, 'arc'), may hold values from 0 to 8191, as said below
- base_cost: float32 [16, 8192], P(None, 'arc'), may hold values from 0.05 to 1
- arc_price: float32 [16, 8192], P(None, 'arc'), may hold values from 0 to 1
- capacity: float32 [16, 8192], P(None, 'arc')
- path_arcs: int32 [1024, 128], P(('comm', 'arc')), may hold values from 0 to 131071, as said below
- demand: float32 [1024], P(('comm', 'arc')), may hold values from 0.5 to 2
Outputs:
- final_dist: float32 [1024, 8192], P('comm', 'arc')
- new_price: float32 [16, 8192], P(None, 'arc')
The draws below stay inside these ranges and needn't reach their ends.
Inputs may be any that keep to these rules, and one draw needn't show every extreme that they name: `arc_tail`: the tail of arc s * 8192 + v lies in a node block (nodes 128 b to 128 b + 127) at most 2 blocks before or after v's block, counted around the cycle of blocks. Row k is a walk: the head of path_arcs[k, h + 1] (its id modulo 8192) is the tail of path_arcs[k, h]. `source_node`: the tail of path_arcs[k, 127].
All inputs are finite; a program needn't handle non-finite values.
Results may differ from the reference program's by a relative error of at most 0.00002.
Values sent between devices are 32-bit elements; how exact they have to be, the bound alone decides.
A program may use at most 64 MiB of HBM per device.

```python
import math
import jax
import jax.numpy as jnp
from jax import lax

LANES = 128
BLK_DEV = 2
IN_DEG = 16
SWEEPS = 8
HOPS = 128
NODES = 8192
K = 1024


def make_tails(key):
    tail_key = jax.random.fold_in(key, 11)
    key_pair = jax.random.split(tail_key, 2)
    head_nodes = jnp.arange(NODES, dtype=jnp.int32)
    head_block = head_nodes // LANES
    blocks_all = NODES // LANES
    offset = jax.random.randint(key_pair[0], (IN_DEG, NODES), -BLK_DEV, BLK_DEV + 1)
    lane_pick = jax.random.randint(key_pair[1], (IN_DEG, NODES), 0, LANES)
    return (jnp.mod(head_block[None, :] + offset, blocks_all) * LANES + lane_pick).astype(jnp.int32)


def make_walks(key):
    tail_nodes = make_tails(key).reshape(-1)
    walk_key = jax.random.fold_in(key, 23)
    key_pair = jax.random.split(walk_key, 2)
    sink_nodes = jax.random.randint(key_pair[0], (K,), 0, NODES).astype(jnp.int32)
    slot_picks = jax.random.randint(key_pair[1], (HOPS, K), 0, IN_DEG).astype(jnp.int32)

    def advance(current, picked):
        arc_ids = picked * NODES + current
        return (tail_nodes[arc_ids], arc_ids)
    endpoint, walked = lax.scan(advance, sink_nodes, slot_picks)
    return (walked.T.astype(jnp.int32), endpoint.astype(jnp.int32))


def draw_arc_tail(key, part):
    return make_tails(key)


def draw_path_arcs(key, part):
    return make_walks(key)[0]


def draw_source_node(key, part):
    return make_walks(key)[1]


def draw_capacity(key, part):
    positions = jnp.arange(NODES, dtype=jnp.float32) / NODES
    rough_factor = jnp.exp(jax.random.uniform(key, (IN_DEG, NODES), jnp.float32, math.log(0.3), math.log(3.0)))
    return (rough_factor * (0.5 + 1.5 * positions)[None, :]).astype(jnp.float32)


def block_scale(own_key, dims, pieces, least, largest):
    loudness = 1.0
    for dim, parts in pieces:
        heights = jax.random.uniform(jax.random.fold_in(jax.random.fold_in(own_key, 6), dim), (parts,), jnp.float32, least / len(pieces), largest / len(pieces))
        loudness = loudness * jnp.repeat(jnp.exp(heights), dims[dim] // parts).reshape((-1,) + (1,) * (len(dims) - 1 - dim))
    return loudness


def setup_inputs(seed: int = 0) -> dict:
    key_of = jax.random.split(jax.random.key(seed), 9)
    return {
        "prev_dist": jnp.clip(4.0 * jax.random.uniform(key_of[0], (K, NODES), jnp.float32) ** block_scale(key_of[0], (K, NODES), ((0, 8), (1, 32)), -0.2, 0.2), 0.0, 4.0),
        "source_node": draw_source_node(jax.random.fold_in(key_of[8], 71), 0),
        "arc_tail": draw_arc_tail(jax.random.fold_in(key_of[8], 71), 0),
        "base_cost": jnp.clip(jnp.exp(math.log(1.0) - 2.9957323 * jax.random.uniform(key_of[3], (IN_DEG, NODES), jnp.float32) ** block_scale(key_of[3], (IN_DEG, NODES), ((1, 32),), -0.2, 0.2)), 0.05, 1.0),
        "arc_price": jnp.clip(1.0 * jax.random.uniform(key_of[4], (IN_DEG, NODES), jnp.float32) ** block_scale(key_of[4], (IN_DEG, NODES), ((1, 32),), -0.2, 0.2), 0.0, 1.0),
        "capacity": draw_capacity(jax.random.fold_in(key_of[8], 71), 0),
        "path_arcs": draw_path_arcs(jax.random.fold_in(key_of[8], 71), 0),
        "demand": jnp.clip(jnp.exp(math.log(2.0) - 1.3862944 * jax.random.uniform(key_of[7], (K,), jnp.float32) ** block_scale(key_of[7], (K,), ((0, 256),), -0.2, 0.2)), 0.5, 2.0),
    }


step_size = 0.25
eps_value = 1e-06

def reference(prev_dist, source_node, arc_tail, base_cost, arc_price, capacity, path_arcs, demand):
    arc_weight = base_cost + arc_price
    node_ids = jnp.arange(NODES, dtype=jnp.int32)
    distance = jnp.where(node_ids[None, :] == source_node[:, None], jnp.float32(0.0), prev_dist)
    for sweep_number in range(SWEEPS):
        best_dist = distance
        for in_slot in range(IN_DEG):
            candidate = jnp.take(distance, arc_tail[in_slot], axis=1) + arc_weight[in_slot][None, :]
            best_dist = jnp.minimum(best_dist, candidate)
        distance = best_dist
    amounts = jnp.broadcast_to(demand[:, None], path_arcs.shape).reshape(-1)
    flattened = jnp.zeros((IN_DEG * NODES,), jnp.float32).at[path_arcs.reshape(-1)].add(amounts)
    arc_flow = flattened.reshape(IN_DEG, NODES)
    gradient = arc_flow - capacity
    scale_root = jnp.sqrt(jnp.sum(gradient * gradient) / (IN_DEG * NODES) + eps_value)
    new_price = jnp.maximum(arc_price + step_size * gradient / scale_root, jnp.float32(0.0))
    return (distance, new_price)
```

```python
import functools

import jax
import jax.numpy as jnp
from jax import lax
from jax.experimental import pallas as pl
from jax.experimental.pallas import tpu as pltpu
from jax.sharding import PartitionSpec as P

SWEEPS = 8
LANES = 128
MESH = pl.DeviceIdType.MESH
F32 = jnp.float32
BF16 = jnp.bfloat16

step_size = 0.25
eps_value = 1e-06


def parts(x):
    high = x.astype(BF16)
    return high, (x - high.astype(F32)).astype(BF16)


def peer_of(axis, size, step):
    return lax.rem(lax.axis_index(axis) + step, size)


def kernel(
    arcs, comms, nodes,
    dist_ref, source_ref, tail_ref, cost_ref, price_ref, cap_ref, path_ref, demand_ref,
    dist_out, price_out,
    own, left, right, best, lhs, hot, rel, weight,
    pay, routes, ends, picks, flow, flows, square, squares,
    near_send, near_recv, pay_send, pay_recv, flow_send, flow_recv, square_send, square_recv,
):
    me = lax.axis_index("arc")
    group = lax.axis_index("comm")
    span = 2 * LANES
    first = me * span
    after = lax.rem(me + 1, arcs)
    before = lax.rem(me + arcs - 1, arcs)

    barrier = pltpu.get_barrier_semaphore()

    @pl.loop(1, arcs)
    def _(step):
        pl.semaphore_signal(
            barrier, inc=1, device_id={"arc": peer_of("arc", arcs, step)}, device_id_type=MESH
        )

    @pl.loop(1, comms)
    def _(step):
        pl.semaphore_signal(
            barrier, inc=1, device_id={"comm": peer_of("comm", comms, step)}, device_id_type=MESH
        )

    source = jnp.broadcast_to(source_ref[...], (LANES, LANES)).T
    lane = lax.broadcasted_iota(jnp.int32, (LANES, LANES), 1)
    for b in range(2):
        block = dist_ref[:, b * LANES : (b + 1) * LANES]
        own[0, b] = jnp.where(source == lane + (first + b * LANES), F32(0.0), block)

    pay[0:4, :] = path_ref[...].astype(F32)
    for r in range(4):
        pay[4 + r : 5 + r, :] = jnp.full((1, LANES), demand_ref[r], F32)

    arc_weight = cost_ref[...] + price_ref[...]
    shifted = tail_ref[...] - (first - span)
    shifted = jnp.where(shifted < 0, shifted + nodes, shifted)
    shifted = jnp.where(shifted >= nodes, shifted - nodes, shifted)
    for h in range(2):
        cols = slice(h * LANES, (h + 1) * LANES)
        pair = jnp.concatenate([shifted[0:8, cols], shifted[8:16, cols]], axis=1)
        cost = jnp.concatenate([arc_weight[0:8, cols], arc_weight[8:16, cols]], axis=1)
        rel[h] = pair
        at = pair // LANES
        inside = (at == 2) | (at == 3)
        near = (at == 1) | (at == 4)
        weight[0, h] = jnp.where(inside, cost, jnp.inf)
        weight[1, h] = jnp.where(near, cost, jnp.inf)
        weight[2, h] = jnp.where(inside | near, jnp.inf, cost)

    row = lax.broadcasted_iota(jnp.int32, (LANES, span), 0)

    @pl.loop(0, 8)
    def _(t):
        for h in range(2):
            want = jnp.broadcast_to(rel[h, pl.ds(t, 1), :], (LANES, span))
            for k, at in enumerate((2, 3, 1, 4, 0 if h == 0 else 5)):
                one = jnp.where(want == row + at * LANES, F32(1.0), F32(0.0)).astype(BF16)
                hot[h, t, k * span : k * span + LANES, :] = one
                hot[h, t, k * span + LANES : (k + 1) * span, :] = one

    pl.semaphore_wait(barrier, arcs + comms - 2)

    def near_copies(slot):
        out = []
        for k, (b, there, target) in enumerate(
            ((1, left, after), (0, right, before), (0, left, after), (1, right, before))
        ):
            out.append(
                pltpu.make_async_remote_copy(
                    src_ref=own.at[slot, b],
                    dst_ref=there.at[slot, b],
                    send_sem=near_send.at[slot, k],
                    recv_sem=near_recv.at[slot, k],
                    device_id={"arc": target},
                    device_id_type=MESH,
                )
            )
        return out

    def spread(axis, size, source_ref_, target_ref, send, recv):
        mine = lax.axis_index(axis)

        def copy(peer, slot):
            return pltpu.make_async_remote_copy(
                src_ref=source_ref_,
                dst_ref=target_ref.at[slot],
                send_sem=send.at[peer],
                recv_sem=recv.at[slot],
                device_id={axis: peer},
                device_id_type=MESH,
            )

        def start():
            @pl.loop(1, size)
            def _(step):
                copy(peer_of(axis, size, step), mine).start()

        def finish():
            @pl.loop(1, size)
            def _(step):
                peer = peer_of(axis, size, step)
                copy(peer, mine).wait_send()
                copy(peer, peer).wait_recv()

        return start, finish

    send_pay, get_pay = spread("arc", arcs, pay, routes, pay_send, pay_recv)
    send_flow, get_flow = spread("comm", comms, flow, flows, flow_send, flow_recv)
    send_square, get_square = spread("arc", arcs, square, squares, square_send, square_recv)

    def phase(p, h, start, width, best_dist):
        cols = slice(start, start + width)
        rows = slice((0, 512, 1024)[p], (0, 512, 1024)[p] + width)
        for t in range(8):
            found = jnp.dot(lhs[:, cols], hot[h, t, rows, :], preferred_element_type=F32)
            found = found + weight[p, h, t : t + 1, :]
            best_dist = jnp.minimum(best_dist, jnp.minimum(found[:, :LANES], found[:, LANES:]))
        return best_dist

    def put(place, block):
        high, low = parts(block)
        lhs[:, place * span : place * span + LANES] = high
        lhs[:, place * span + LANES : (place + 1) * span] = low

    def histogram():
        get_pay()
        routes[me] = pay[...]
        node_row = lax.broadcasted_iota(jnp.int32, (span, LANES), 0)
        slot_row = lax.broadcasted_iota(jnp.int32, (16, LANES), 0)

        def chunk(c, total):
            for i in range(8):
                for r in range(4):
                    at = slice((i * 4 + r) * LANES, (i * 4 + r + 1) * LANES)
                    ids = routes[c * 8 + i, r : r + 1, :].astype(jnp.int32)
                    amount = routes[c * 8 + i, 4 + r : 5 + r, :]
                    node = jnp.broadcast_to((ids & (nodes - 1)) - first, (span, LANES))
                    hop_slot = jnp.broadcast_to(ids // nodes, (16, LANES))
                    ends[:, at] = jnp.where(node == node_row, F32(1.0), F32(0.0)).astype(BF16)
                    given = jnp.where(hop_slot == slot_row, amount, F32(0.0))
                    high, low = parts(given)
                    picks[0:16, at] = high
                    picks[16:32, at] = low
            return total + lax.dot_general(
                picks[...], ends[...], (((1,), (1,)), ((), ())), preferred_element_type=F32
            )

        total = lax.fori_loop(0, arcs // 8, chunk, jnp.zeros((32, span), F32))
        flow[...] = total[0:16] + total[16:32]
        flows[group] = flow[...]
        send_flow()

    def squares_out():
        get_flow()
        total = flows[0]
        for z in range(1, comms):
            total = total + flows[z]
        gradient = total - cap_ref[...]
        flow[...] = gradient
        sq = gradient * gradient
        square[...] = (sq[0:8, :LANES] + sq[8:16, :LANES]) + (sq[0:8, LANES:] + sq[8:16, LANES:])
        squares[me] = square[...]
        send_square()

    def prices():
        get_square()
        total = squares[0]
        for a in range(1, arcs):
            total = total + squares[a]
        whole = jnp.sum(total, axis=(0, 1), keepdims=True)
        root = jnp.sqrt(whole / F32(16 * nodes) + F32(eps_value))
        price_out[...] = jnp.maximum(
            price_ref[...] + F32(step_size) * flow[...] / root, F32(0.0)
        )

    @pl.loop(0, SWEEPS)
    def _(sweep):
        slot = lax.rem(sweep, 2)
        copies = near_copies(slot)
        for copy in copies:
            copy.start()
        pl.when(sweep == 0)(send_pay)
        for b in range(2):
            put(b, own[slot, b])
        for h in range(2):
            best[h] = phase(0, h, 0, 512, own[slot, h])
        pl.when(sweep == 1)(histogram)
        pl.when(sweep == 3)(squares_out)
        pl.when(sweep == 5)(prices)
        copies[0].wait_recv()
        copies[1].wait_recv()
        put(2, left[slot, 1])
        put(3, right[slot, 0])
        for h in range(2):
            best[h] = phase(1, h, 512, 512, best[h])
        copies[2].wait_recv()
        copies[3].wait_recv()
        put(4, left[slot, 0])
        put(5, right[slot, 1])
        for copy in copies:
            copy.wait_send()
        for h in range(2):
            own[1 - slot, h] = phase(2, h, 1024 + h * span, span, best[h])

    for b in range(2):
        dist_out[:, b * LANES : (b + 1) * LANES] = own[SWEEPS % 2, b]


def shards(prev_dist, source_node, arc_tail, base_cost, arc_price, capacity, path_arcs, demand):
    arcs = lax.axis_size("arc")
    comms = lax.axis_size("comm")
    rows, span = prev_dist.shape
    vmem = pl.BlockSpec(memory_space=pltpu.VMEM)
    smem = pl.BlockSpec(memory_space=pltpu.SMEM)
    dma = pltpu.SemaphoreType.DMA
    return pl.pallas_call(
        functools.partial(kernel, arcs, comms, arcs * span),
        out_shape=(
            jax.ShapeDtypeStruct(prev_dist.shape, F32),
            jax.ShapeDtypeStruct(arc_price.shape, F32),
        ),
        in_specs=[vmem] * 7 + [smem],
        out_specs=(vmem, vmem),
        scratch_shapes=[
            pltpu.VMEM((2, 2, rows, LANES), F32),
            pltpu.VMEM((2, 2, rows, LANES), F32),
            pltpu.VMEM((2, 2, rows, LANES), F32),
            pltpu.VMEM((2, rows, LANES), F32),
            pltpu.VMEM((rows, 12 * LANES), BF16),
            pltpu.VMEM((2, 8, 10 * LANES, span), BF16),
            pltpu.VMEM((2, 8, span), jnp.int32),
            pltpu.VMEM((3, 2, 8, span), F32),
            pltpu.VMEM((8, LANES), F32),
            pltpu.VMEM((arcs, 8, LANES), F32),
            pltpu.VMEM((span, 32 * LANES), BF16),
            pltpu.VMEM((32, 32 * LANES), BF16),
            pltpu.VMEM((16, span), F32),
            pltpu.VMEM((comms, 16, span), F32),
            pltpu.VMEM((8, LANES), F32),
            pltpu.VMEM((arcs, 8, LANES), F32),
            dma((2, 4)),
            dma((2, 4)),
            dma((arcs,)),
            dma((arcs,)),
            dma((comms,)),
            dma((comms,)),
            dma((arcs,)),
            dma((arcs,)),
        ],
        compiler_params=pltpu.CompilerParams(
            collective_id=0, has_side_effects=True, vmem_limit_bytes=48 * 1024 * 1024
        ),
    )(
        prev_dist, source_node.reshape(1, rows), arc_tail, base_cost, arc_price, capacity,
        path_arcs, demand,
    )


def solution(mesh):
    in_specs = (
        P("comm", "arc"),
        P("comm"),
        P(None, "arc"),
        P(None, "arc"),
        P(None, "arc"),
        P(None, "arc"),
        P(("comm", "arc"), None),
        P(("comm", "arc")),
    )
    out_specs = (P("comm", "arc"), P(None, "arc"))
    return jax.shard_map(shards, mesh=mesh, in_specs=in_specs, out_specs=out_specs, check_vma=False)
```

```python
import functools

import jax
import jax.numpy as jnp
from jax import lax
from jax.experimental import pallas as pl
from jax.experimental.pallas import tpu as pltpu
from jax.sharding import PartitionSpec as P

SWEEPS = 8
CHUNKS = 2

LANES = 128
MESH = pl.DeviceIdType.MESH
F32 = jnp.float32
BF16 = jnp.bfloat16
HOT = jnp.float8_e4m3fn
ROW = 8

step_size = 0.25
eps_value = 1e-06


def parts(x):
    high = x.astype(BF16)
    return high, (x - high.astype(F32)).astype(BF16)


def kernel(
    arcs, comms, nodes,
    dist_hbm, source_hbm, tail_hbm, cost_hbm, price_hbm, cap_hbm, path_hbm, demand_ref,
    dist_out, price_out,
    dist_ref, source_ref, tail_ref, cost_ref, price_ref, cap_ref, path_ref, fetch_sem,
    own, left, right, best, lhs, hot, rel, weight,
    pay, routes, ends, picks, flow, flows, square, squares, square_sum, square_sums,
    near_send, near_recv, row_send, row_recv, col_send, col_recv, flow_send, flow_recv,
):
    me = lax.axis_index("arc")
    group = lax.axis_index("comm")
    span = 2 * LANES
    rows = LANES // CHUNKS
    first = me * span
    after = lax.rem(me + 1, arcs)
    before = lax.rem(me + arcs - 1, arcs)

    barrier = pltpu.get_barrier_semaphore()
    fetches = [
        pltpu.make_async_copy(there, here, fetch_sem.at[k])
        for k, (there, here) in enumerate(
            (
                (tail_hbm, tail_ref),
                (cost_hbm, cost_ref),
                (price_hbm, price_ref),
                (source_hbm, source_ref),
                (dist_hbm, dist_ref),
                (path_hbm, path_ref),
                (cap_hbm, cap_ref),
            )
        )
    ]
    for fetch in fetches:
        fetch.start()

    line = me // ROW
    place = lax.rem(me, ROW)
    lines = arcs // ROW

    def row_peer(step):
        return line * ROW + lax.rem(place + step, ROW)

    def col_peer(step):
        return lax.rem(line + step, lines) * ROW + place

    def ring(step):
        return lax.rem(group + comms + step, comms)

    greeted = [("arc", row_peer(step)) for step in range(1, ROW)]
    greeted += [("arc", col_peer(step)) for step in range(1, lines)]
    greeted += [("arc", after), ("arc", before)]
    greeted += [("comm", ring(step)) for step in (1, 2, -1, -2)]
    for axis, peer in greeted:
        pl.semaphore_signal(barrier, inc=1, device_id={axis: peer}, device_id_type=MESH)

    for fetch in fetches:
        fetch.wait()

    source = jnp.broadcast_to(source_ref[...], (LANES, LANES)).T
    lane = lax.broadcasted_iota(jnp.int32, (LANES, LANES), 1)
    for b in range(2):
        block = dist_ref[:, b * LANES : (b + 1) * LANES]
        block = jnp.where(source == lane + (first + b * LANES), F32(0.0), block)
        for c in range(CHUNKS):
            own[0, c, b] = block[c * rows : (c + 1) * rows]

    pay[0:4, :] = path_ref[...].astype(F32)
    for r in range(4):
        pay[4 + r : 5 + r, :] = jnp.full((1, LANES), demand_ref[r], F32)

    arc_weight = cost_ref[...] + price_ref[...]
    shifted = tail_ref[...] - (first - span)
    shifted = jnp.where(shifted < 0, shifted + nodes, shifted)
    shifted = jnp.where(shifted >= nodes, shifted - nodes, shifted)
    for h in range(2):
        cols = slice(h * LANES, (h + 1) * LANES)
        pair = jnp.concatenate([shifted[0:8, cols], shifted[8:16, cols]], axis=1)
        cost = jnp.concatenate([arc_weight[0:8, cols], arc_weight[8:16, cols]], axis=1)
        rel[h] = pair
        at = pair // LANES
        inside = (at == 2) | (at == 3)
        near = (at == 1) | (at == 4)
        weight[0, h] = jnp.where(inside, cost, jnp.inf)
        weight[1, h] = jnp.where(near, cost, jnp.inf)
        weight[2, h] = jnp.where(inside | near, jnp.inf, cost)

    row = lax.broadcasted_iota(jnp.int32, (LANES, span), 0)

    @pl.loop(0, 8)
    def _(t):
        for h in range(2):
            want = jnp.broadcast_to(rel[h, pl.ds(t, 1), :], (LANES, span))
            for k, at in enumerate((2, 3, 1, 4, 0 if h == 0 else 5)):
                one = jnp.where(want == row + at * LANES, F32(1.0), F32(0.0)).astype(HOT)
                hot[h, t, k * span : k * span + LANES, :] = one
                hot[h, t, k * span + LANES : (k + 1) * span, :] = one

    pl.semaphore_wait(barrier, len(greeted))

    def near_copies(slot, c):
        out = []
        for k, (b, there, target) in enumerate(
            ((1, left, after), (0, right, before), (0, left, after), (1, right, before))
        ):
            out.append(
                pltpu.make_async_remote_copy(
                    src_ref=own.at[slot, c, b],
                    dst_ref=there.at[slot, c, b],
                    send_sem=near_send.at[slot, c, k],
                    recv_sem=near_recv.at[slot, c, k],
                    device_id={"arc": target},
                    device_id_type=MESH,
                )
            )
        return out

    def row_copies(kind, source_at, target_at):
        return [
            pltpu.make_async_remote_copy(
                src_ref=source_at,
                dst_ref=target_at,
                send_sem=row_send.at[kind, step],
                recv_sem=row_recv.at[kind, step],
                device_id={"arc": row_peer(step)},
                device_id_type=MESH,
            )
            for step in range(1, ROW)
        ]

    def col_copies(kind, source_at, target_at):
        return [
            pltpu.make_async_remote_copy(
                src_ref=source_at,
                dst_ref=target_at,
                send_sem=col_send.at[kind, step],
                recv_sem=col_recv.at[kind, step],
                device_id={"arc": col_peer(step)},
                device_id_type=MESH,
            )
            for step in range(1, lines)
        ]

    def flow_copies(moves):
        return [
            pltpu.make_async_remote_copy(
                src_ref=flow if of is None else flows.at[ring(of)],
                dst_ref=flows.at[ring(0 if of is None else of)],
                send_sem=flow_send.at[k],
                recv_sem=flow_recv.at[k],
                device_id={"comm": ring(step)},
                device_id_type=MESH,
            )
            for k, of, step in moves
        ]

    mine = routes.at[pl.ds(pl.multiple_of(line * ROW, ROW), ROW)]
    row_pay = row_copies(0, pay, routes.at[me])
    col_pay = col_copies(0, mine, mine)
    near_flow = flow_copies([(0, None, 1), (1, None, 2), (2, None, -1), (3, None, -2)])
    far_flow = flow_copies([(4, 1, -2), (5, 2, -2), (6, -1, 2)])
    row_square = row_copies(1, square, squares.at[place])
    col_square = col_copies(1, square_sum, square_sums.at[line])

    def start(copies):
        for copy in copies:
            copy.start()

    def finish(copies):
        for copy in copies:
            copy.wait_send()
        for copy in copies:
            copy.wait_recv()

    def phase(p, c, h, start, width, best_dist):
        cols = slice(start, start + width)
        taken = slice((0, 512, 1024)[p], (0, 512, 1024)[p] + width)
        for t in range(8):
            found = jnp.dot(lhs[c, :, cols], hot[h, t, taken, :], preferred_element_type=F32)
            found = found + weight[p, h, t : t + 1, :]
            best_dist = jnp.minimum(best_dist, jnp.minimum(found[:, :LANES], found[:, LANES:]))
        return best_dist

    def put(c, place, block):
        high, low = parts(block)
        lhs[c, :, place * span : place * span + LANES] = high
        lhs[c, :, place * span + LANES : (place + 1) * span] = low

    def count_line(step):
        node_row = lax.broadcasted_iota(jnp.int32, (span, LANES), 0)
        slot_row = lax.broadcasted_iota(jnp.int32, (16, LANES), 0)
        base = lax.rem(line + step, lines) * ROW
        for i in range(ROW):
            for r in range(4):
                at = slice((i * 4 + r) * LANES, (i * 4 + r + 1) * LANES)
                ids = routes[base + i, r : r + 1, :].astype(jnp.int32)
                amount = routes[base + i, 4 + r : 5 + r, :]
                node = jnp.broadcast_to((ids & (nodes - 1)) - first, (span, LANES))
                hop_slot = jnp.broadcast_to(ids // nodes, (16, LANES))
                ends[:, at] = jnp.where(node == node_row, F32(1.0), F32(0.0)).astype(BF16)
                given = jnp.where(hop_slot == slot_row, amount, F32(0.0))
                high, low = parts(given)
                picks[0:16, at] = high
                picks[16:32, at] = low
        both = lax.dot_general(
            picks[...], ends[...], (((1,), (1,)), ((), ())), preferred_element_type=F32
        )
        return both[0:16] + both[16:32]

    def flow_step(t):
        if t == 0:
            finish(row_pay)
            routes[me] = pay[...]
            start(col_pay)
        if t == 1:
            flow[...] = count_line(0)
        if t == 2:
            finish(col_pay)

            @pl.loop(1, 3)
            def _(step):
                flow[...] += count_line(step)
        if t == 3:
            flow[...] += count_line(3)
            flows[group] = flow[...]
            start(near_flow)
        if t == 4:
            finish(near_flow)
            start(far_flow)
        if t == 5:
            finish(far_flow)
            total = flows[0]
            for z in range(1, comms):
                total = total + flows[z]
            gradient = total - cap_ref[...]
            flow[...] = gradient
            sq = gradient * gradient
            square[...] = (sq[0:8, :LANES] + sq[8:16, :LANES]) + (sq[0:8, LANES:] + sq[8:16, LANES:])
            start(row_square)
        if t == 6:
            finish(row_square)
            squares[place] = square[...]
            total = squares[0]
            for a in range(1, ROW):
                total = total + squares[a]
            square_sum[...] = total
            start(col_square)
        if t == 7:
            finish(col_square)
            square_sums[line] = square_sum[...]
            total = square_sums[0]
            for a in range(1, lines):
                total = total + square_sums[a]
            whole = jnp.sum(total, axis=(0, 1), keepdims=True)
            root = jnp.sqrt(whole / F32(16 * nodes) + F32(eps_value))
            price_out[...] = jnp.maximum(
                price_ref[...] + F32(step_size) * flow[...] / root, F32(0.0)
            )

    def send(slot, c):
        start(near_copies(slot, c))

    def inner(slot, c):
        for b in range(2):
            put(c, b, own[slot, c, b])
        for h in range(2):
            best[c, h] = phase(0, c, h, 0, 512, own[slot, c, h])

    def outer(slot, c):
        copies = near_copies(slot, c)
        copies[0].wait_recv()
        copies[1].wait_recv()
        put(c, 2, left[slot, c, 1])
        put(c, 3, right[slot, c, 0])
        for h in range(2):
            best[c, h] = phase(1, c, h, 512, 512, best[c, h])
        copies[2].wait_recv()
        copies[3].wait_recv()
        put(c, 4, left[slot, c, 0])
        put(c, 5, right[slot, c, 1])
        for copy in copies:
            copy.wait_send()
        for h in range(2):
            own[1 - slot, c, h] = phase(2, c, h, 1024 + h * span, span, best[c, h])

    for c in range(CHUNKS):
        send(0, c)
    start(row_pay)

    @pl.loop(0, SWEEPS)
    def _(sweep):
        slot = lax.rem(sweep, 2)
        for c in range(CHUNKS):
            inner(slot, c)
        for t in range(SWEEPS):
            pl.when(sweep == t)(functools.partial(flow_step, t))
        for c in range(CHUNKS):
            outer(slot, c)

            @pl.when(sweep < SWEEPS - 1)
            def _():
                send(1 - slot, c)

    for c in range(CHUNKS):
        for b in range(2):
            dist_out[c * rows : (c + 1) * rows, b * LANES : (b + 1) * LANES] = own[SWEEPS % 2, c, b]


def shards(prev_dist, source_node, arc_tail, base_cost, arc_price, capacity, path_arcs, demand):
    arcs = lax.axis_size("arc")
    comms = lax.axis_size("comm")
    rows, span = prev_dist.shape
    vmem = pl.BlockSpec(memory_space=pltpu.VMEM)
    smem = pl.BlockSpec(memory_space=pltpu.SMEM)
    dma = pltpu.SemaphoreType.DMA
    return pl.pallas_call(
        functools.partial(kernel, arcs, comms, arcs * span),
        out_shape=(
            pltpu.VMEM(prev_dist.shape, F32),
            pltpu.VMEM(arc_price.shape, F32),
        ),
        in_specs=[pl.BlockSpec(memory_space=pltpu.HBM)] * 7 + [smem],
        out_specs=(vmem, vmem),
        scratch_shapes=[
            pltpu.VMEM(prev_dist.shape, F32),
            pltpu.VMEM((1, rows), jnp.int32),
            pltpu.VMEM(arc_tail.shape, jnp.int32),
            pltpu.VMEM(arc_price.shape, F32),
            pltpu.VMEM(arc_price.shape, F32),
            pltpu.VMEM(arc_price.shape, F32),
            pltpu.VMEM(path_arcs.shape, jnp.int32),
            dma((7,)),
            pltpu.VMEM((2, CHUNKS, 2, rows // CHUNKS, LANES), F32),
            pltpu.VMEM((2, CHUNKS, 2, rows // CHUNKS, LANES), F32),
            pltpu.VMEM((2, CHUNKS, 2, rows // CHUNKS, LANES), F32),
            pltpu.VMEM((CHUNKS, 2, rows // CHUNKS, LANES), F32),
            pltpu.VMEM((CHUNKS, rows // CHUNKS, 12 * LANES), BF16),
            pltpu.VMEM((2, 8, 10 * LANES, span), HOT),
            pltpu.VMEM((2, 8, span), jnp.int32),
            pltpu.VMEM((3, 2, 8, span), F32),
            pltpu.VMEM((8, LANES), F32),
            pltpu.VMEM((arcs, 8, LANES), F32),
            pltpu.VMEM((span, 32 * LANES), BF16),
            pltpu.VMEM((32, 32 * LANES), BF16),
            pltpu.VMEM((16, span), F32),
            pltpu.VMEM((comms, 16, span), F32),
            pltpu.VMEM((8, LANES), F32),
            pltpu.VMEM((ROW, 8, LANES), F32),
            pltpu.VMEM((8, LANES), F32),
            pltpu.VMEM((arcs // ROW, 8, LANES), F32),
            dma((2, CHUNKS, 4)),
            dma((2, CHUNKS, 4)),
            dma((2, ROW)),
            dma((2, ROW)),
            dma((2, arcs // ROW)),
            dma((2, arcs // ROW)),
            dma((7,)),
            dma((7,)),
        ],
        compiler_params=pltpu.CompilerParams(
            collective_id=0, has_side_effects=True, vmem_limit_bytes=63 * 1024 * 1024 - 65536
        ),
    )(
        prev_dist, source_node.reshape(1, rows), arc_tail, base_cost, arc_price, capacity,
        path_arcs, demand,
    )


def solution(mesh):
    in_specs = (
        P("comm", "arc"),
        P("comm"),
        P(None, "arc"),
        P(None, "arc"),
        P(None, "arc"),
        P(None, "arc"),
        P(("comm", "arc"), None),
        P(("comm", "arc")),
    )
    out_specs = (P("comm", "arc"), P(None, "arc"))
    return jax.shard_map(shards, mesh=mesh, in_specs=in_specs, out_specs=out_specs, check_vma=False)
```

```python
import functools

import jax
import jax.numpy as jnp
from jax import lax
from jax.experimental import pallas as pl
from jax.experimental.pallas import tpu as pltpu
from jax.sharding import PartitionSpec as P

SWEEPS = 8
CHUNKS = 2

LANES = 128
MESH = pl.DeviceIdType.MESH
F32 = jnp.float32
BF16 = jnp.bfloat16
HOT = jnp.float8_e4m3fn
ROW = 8

step_size = 0.25
eps_value = 1e-06


def parts(x):
    high = x.astype(BF16)
    return high, (x - high.astype(F32)).astype(BF16)


def kernel(
    arcs, comms, nodes,
    dist_hbm, source_hbm, tail_hbm, cost_hbm, price_hbm, cap_hbm, path_hbm, demand_ref,
    dist_out, price_out,
    dist_ref, source_ref, tail_ref, cost_ref, price_ref, cap_ref, path_ref, fetch_sem,
    own, reduced, beside, across, missing, best, lhs, hot, seen, rel, weight, tell, told,
    pay, routes, ends, picks, flow, flows, square, squares, square_sum, square_sums,
    near_send, near_recv, tell_send, tell_recv, row_send, row_recv, col_send, col_recv, flow_send, flow_recv,
):
    me = lax.axis_index("arc")
    group = lax.axis_index("comm")
    span = 2 * LANES
    rows = LANES // CHUNKS
    first = me * span
    after = lax.rem(me + 1, arcs)
    before = lax.rem(me + arcs - 1, arcs)

    barrier = pltpu.get_barrier_semaphore()
    fetches = [
        pltpu.make_async_copy(there, here, fetch_sem.at[k])
        for k, (there, here) in enumerate(
            (
                (tail_hbm, tail_ref),
                (cost_hbm, cost_ref),
                (price_hbm, price_ref),
                (source_hbm, source_ref),
                (dist_hbm, dist_ref),
                (path_hbm, path_ref),
                (cap_hbm, cap_ref),
            )
        )
    ]
    for fetch in fetches:
        fetch.start()

    core = lax.rem(me, 2)
    partner = me + 1 - 2 * core
    other = lax.rem(me + arcs - 1 + 2 * core, arcs)
    line = me // ROW
    place = lax.rem(me, ROW)
    lines = arcs // ROW

    def row_peer(step):
        return line * ROW + lax.rem(place + step, ROW)

    def col_peer(step):
        return lax.rem(line + step, lines) * ROW + place

    def ring(step):
        return lax.rem(group + comms + step, comms)

    greeted = [("arc", row_peer(step)) for step in range(1, ROW)]
    greeted += [("arc", col_peer(step)) for step in range(1, lines)]
    greeted += [("arc", after), ("arc", before)]
    greeted += [("comm", ring(step)) for step in (1, 2, -1, -2)]
    for axis, peer in greeted:
        pl.semaphore_signal(barrier, inc=1, device_id={axis: peer}, device_id_type=MESH)

    for fetch in fetches:
        fetch.wait()

    source = jnp.broadcast_to(source_ref[...], (LANES, LANES)).T
    lane = lax.broadcasted_iota(jnp.int32, (LANES, LANES), 1)
    for b in range(2):
        block = dist_ref[:, b * LANES : (b + 1) * LANES]
        block = jnp.where(source == lane + (first + b * LANES), F32(0.0), block)
        for c in range(CHUNKS):
            own[0, c, b] = block[c * rows : (c + 1) * rows]

    pay[0:4, :] = path_ref[...].astype(F32)
    for r in range(4):
        pay[4 + r : 5 + r, :] = jnp.full((1, LANES), demand_ref[r], F32)

    arc_weight = cost_ref[...] + price_ref[...]
    shifted = tail_ref[...] - (first - span)
    shifted = jnp.where(shifted < 0, shifted + nodes, shifted)
    shifted = jnp.where(shifted >= nodes, shifted - nodes, shifted)
    for h in range(2):
        cols = slice(h * LANES, (h + 1) * LANES)
        pair = jnp.concatenate([shifted[0:8, cols], shifted[8:16, cols]], axis=1)
        cost = jnp.concatenate([arc_weight[0:8, cols], arc_weight[8:16, cols]], axis=1)
        rel[h] = pair
        at = pair // LANES
        inside = (at == 2) | (at == 3)
        low = at < 2
        toward = jnp.where(low, core, 1 - core) == 1
        weight[0, h] = jnp.where(inside, cost, jnp.inf)
        weight[1, h] = jnp.where(inside | ~toward, jnp.inf, cost)
        weight[2, h] = jnp.where(inside | toward, jnp.inf, cost)
        tell[0, h] = pair.astype(F32)
        tell[1, h] = weight[2, h]

    row = lax.broadcasted_iota(jnp.int32, (LANES, span), 0)

    def fill(target, h, t, k, want, at):
        one = jnp.where(want - at * LANES == row, F32(1.0), F32(0.0)).astype(HOT)
        target[h, t, k * span : k * span + LANES, :] = one
        target[h, t, k * span + LANES : (k + 1) * span, :] = one

    @pl.loop(0, 8)
    def _(t):
        for h in range(2):
            want = jnp.broadcast_to(rel[h, pl.ds(t, 1), :], (LANES, span))
            for k, at in enumerate(
                (2, 3, 4 * (1 - core), 4 * (1 - core) + 1, 4 * core, 4 * core + 1)
            ):
                fill(hot, h, t, k, want, at)

    for k in range(2):
        for c in range(CHUNKS):
            for b in range(2):
                missing[k, c, b] = jnp.full((rows, LANES), jnp.inf, F32)

    pl.semaphore_wait(barrier, len(greeted))

    def to_partner(sweep, c):
        return pltpu.make_async_remote_copy(
            src_ref=own.at[sweep, c],
            dst_ref=beside.at[sweep, c],
            send_sem=near_send.at[0, sweep, c],
            recv_sem=near_recv.at[0, sweep, c],
            device_id={"arc": partner},
            device_id_type=MESH,
        )

    def to_other(sweep, c, source_at):
        return pltpu.make_async_remote_copy(
            src_ref=source_at,
            dst_ref=across.at[sweep, c],
            send_sem=near_send.at[1, sweep, c],
            recv_sem=near_recv.at[1, sweep, c],
            device_id={"arc": other},
            device_id_type=MESH,
        )

    arcs_told = pltpu.make_async_remote_copy(
        src_ref=tell,
        dst_ref=told,
        send_sem=tell_send,
        recv_sem=tell_recv,
        device_id={"arc": other},
        device_id_type=MESH,
    )

    def row_copies(kind, source_at, target_at):
        return [
            pltpu.make_async_remote_copy(
                src_ref=source_at,
                dst_ref=target_at,
                send_sem=row_send.at[kind, step],
                recv_sem=row_recv.at[kind, step],
                device_id={"arc": row_peer(step)},
                device_id_type=MESH,
            )
            for step in range(1, ROW)
        ]

    def col_copies(kind, source_at, target_at):
        return [
            pltpu.make_async_remote_copy(
                src_ref=source_at,
                dst_ref=target_at,
                send_sem=col_send.at[kind, step],
                recv_sem=col_recv.at[kind, step],
                device_id={"arc": col_peer(step)},
                device_id_type=MESH,
            )
            for step in range(1, lines)
        ]

    def flow_copies(moves):
        return [
            pltpu.make_async_remote_copy(
                src_ref=flow if of is None else flows.at[ring(of)],
                dst_ref=flows.at[ring(0 if of is None else of)],
                send_sem=flow_send.at[k],
                recv_sem=flow_recv.at[k],
                device_id={"comm": ring(step)},
                device_id_type=MESH,
            )
            for k, of, step in moves
        ]

    mine = routes.at[pl.ds(pl.multiple_of(line * ROW, ROW), ROW)]
    row_pay = row_copies(0, pay, routes.at[me])
    col_pay = col_copies(0, mine, mine)
    near_flow = flow_copies([(0, None, 1), (1, None, 2), (2, None, -1), (3, None, -2)])
    far_flow = flow_copies([(4, 1, -2), (5, 2, -2), (6, -1, 2)])
    row_square = row_copies(1, square, squares.at[place])
    col_square = col_copies(1, square_sum, square_sums.at[line])

    def start(copies):
        for copy in copies:
            copy.start()

    def finish(copies):
        for copy in copies:
            copy.wait_send()
        for copy in copies:
            copy.wait_recv()

    def phase(p, c, h, best_dist):
        for t in range(8):
            found = jnp.dot(
                lhs[c, :, p * 512 : (p + 1) * 512],
                hot[h, t, p * 512 : (p + 1) * 512, :],
                preferred_element_type=F32,
            )
            found = found + weight[p, h, t : t + 1, :]
            best_dist = jnp.minimum(best_dist, jnp.minimum(found[:, :LANES], found[:, LANES:]))
        return best_dist

    def given(c, h):
        best_dist = jnp.full((rows, LANES), jnp.inf, F32)
        for t in range(8):
            found = jnp.dot(lhs[c, :, :512], seen[h, t], preferred_element_type=F32)
            found = found + told[1, h, t : t + 1, :]
            best_dist = jnp.minimum(best_dist, jnp.minimum(found[:, :LANES], found[:, LANES:]))
        return best_dist

    def learn():
        arcs_told.wait_recv()

        @pl.loop(0, 8)
        def _(t):
            for h in range(2):
                want = told[0, h, pl.ds(t, 1), :].astype(jnp.int32)
                want = jnp.broadcast_to(want, (LANES, span))
                for k in range(2):
                    fill(seen, h, t, k, want, 4 * (1 - core) + k)

    def put(c, place, block):
        high, low = parts(block)
        lhs[c, :, place * span : place * span + LANES] = high
        lhs[c, :, place * span + LANES : (place + 1) * span] = low

    def count_line(step):
        node_row = lax.broadcasted_iota(jnp.int32, (span, LANES), 0)
        slot_row = lax.broadcasted_iota(jnp.int32, (16, LANES), 0)
        base = lax.rem(line + step, lines) * ROW
        for i in range(ROW):
            for r in range(4):
                at = slice((i * 4 + r) * LANES, (i * 4 + r + 1) * LANES)
                ids = routes[base + i, r : r + 1, :].astype(jnp.int32)
                amount = routes[base + i, 4 + r : 5 + r, :]
                node = jnp.broadcast_to((ids & (nodes - 1)) - first, (span, LANES))
                hop_slot = jnp.broadcast_to(ids // nodes, (16, LANES))
                ends[:, at] = jnp.where(node == node_row, F32(1.0), F32(0.0)).astype(BF16)
                given = jnp.where(hop_slot == slot_row, amount, F32(0.0))
                high, low = parts(given)
                picks[0:16, at] = high
                picks[16:32, at] = low
        both = lax.dot_general(
            picks[...], ends[...], (((1,), (1,)), ((), ())), preferred_element_type=F32
        )
        return both[0:16] + both[16:32]

    def flow_step(t):
        if t == 0:
            finish(row_pay)
            routes[me] = pay[...]
            start(col_pay)
        if t == 1:
            flow[...] = count_line(0)
        if t == 2:
            finish(col_pay)

            @pl.loop(1, 3)
            def _(step):
                flow[...] += count_line(step)
        if t == 3:
            flow[...] += count_line(3)
            flows[group] = flow[...]
            start(near_flow)
        if t == 4:
            finish(near_flow)
            start(far_flow)
        if t == 5:
            finish(far_flow)
            total = flows[0]
            for z in range(1, comms):
                total = total + flows[z]
            gradient = total - cap_ref[...]
            flow[...] = gradient
            sq = gradient * gradient
            square[...] = (sq[0:8, :LANES] + sq[8:16, :LANES]) + (sq[0:8, LANES:] + sq[8:16, LANES:])
            start(row_square)
        if t == 6:
            finish(row_square)
            squares[place] = square[...]
            total = squares[0]
            for a in range(1, ROW):
                total = total + squares[a]
            square_sum[...] = total
            start(col_square)
        if t == 7:
            finish(col_square)
            square_sums[line] = square_sum[...]
            total = square_sums[0]
            for a in range(1, lines):
                total = total + square_sums[a]
            whole = jnp.sum(total, axis=(0, 1), keepdims=True)
            root = jnp.sqrt(whole / F32(16 * nodes) + F32(eps_value))
            price_out[...] = jnp.maximum(
                price_ref[...] + F32(step_size) * flow[...] / root, F32(0.0)
            )

    for c in range(CHUNKS):
        to_other(0, c, own.at[0, c]).start()
        to_partner(0, c).start()
    arcs_told.start()
    start(row_pay)

    @pl.loop(0, SWEEPS)
    def _(sweep):
        slot = lax.rem(sweep, 2)
        for c in range(CHUNKS):
            for b in range(2):
                put(c, b, own[sweep, c, b])
            for h in range(2):
                best[c, h] = phase(0, c, h, own[sweep, c, h])
        for c in range(CHUNKS):
            to_partner(sweep, c).wait_recv()
            for b in range(2):
                put(c, 2 + b, beside[sweep, c, b])
            for h in range(2):
                reduced[sweep, c, h] = phase(1, c, h, best[c, h])

            @pl.when(sweep < SWEEPS - 1)
            def _():
                to_other(sweep + 1, c, reduced.at[sweep, c]).start()

        pl.when(sweep == 0)(learn)
        for c in range(CHUNKS):
            for h in range(2):
                missing[slot, c, h] = given(c, h)
        for t in range(SWEEPS):
            pl.when(sweep == t)(functools.partial(flow_step, t))
        for c in range(CHUNKS):
            to_other(sweep, c, own.at[0, c]).wait_recv()
            for b in range(2):
                put(c, 4 + b, jnp.minimum(across[sweep, c, b], missing[1 - slot, c, b]))
            for h in range(2):
                own[sweep + 1, c, h] = phase(2, c, h, reduced[sweep, c, h])

            @pl.when(sweep < SWEEPS - 1)
            def _():
                to_partner(sweep + 1, c).start()

    for c in range(CHUNKS):
        for b in range(2):
            dist_out[c * rows : (c + 1) * rows, b * LANES : (b + 1) * LANES] = own[SWEEPS, c, b]

    arcs_told.wait_send()

    @pl.loop(0, SWEEPS)
    def _(sweep):
        for c in range(CHUNKS):
            to_partner(sweep, c).wait_send()
            to_other(sweep, c, own.at[0, c]).wait_send()


def shards(prev_dist, source_node, arc_tail, base_cost, arc_price, capacity, path_arcs, demand):
    arcs = lax.axis_size("arc")
    comms = lax.axis_size("comm")
    rows, span = prev_dist.shape
    vmem = pl.BlockSpec(memory_space=pltpu.VMEM)
    smem = pl.BlockSpec(memory_space=pltpu.SMEM)
    dma = pltpu.SemaphoreType.DMA
    return pl.pallas_call(
        functools.partial(kernel, arcs, comms, arcs * span),
        out_shape=(
            pltpu.VMEM(prev_dist.shape, F32),
            pltpu.VMEM(arc_price.shape, F32),
        ),
        in_specs=[pl.BlockSpec(memory_space=pltpu.HBM)] * 7 + [smem],
        out_specs=(vmem, vmem),
        scratch_shapes=[
            pltpu.VMEM(prev_dist.shape, F32),
            pltpu.VMEM((1, rows), jnp.int32),
            pltpu.VMEM(arc_tail.shape, jnp.int32),
            pltpu.VMEM(arc_price.shape, F32),
            pltpu.VMEM(arc_price.shape, F32),
            pltpu.VMEM(arc_price.shape, F32),
            pltpu.VMEM(path_arcs.shape, jnp.int32),
            dma((7,)),
            pltpu.VMEM((SWEEPS + 1, CHUNKS, 2, rows // CHUNKS, LANES), F32),
            pltpu.VMEM((SWEEPS, CHUNKS, 2, rows // CHUNKS, LANES), F32),
            pltpu.VMEM((SWEEPS, CHUNKS, 2, rows // CHUNKS, LANES), F32),
            pltpu.VMEM((SWEEPS, CHUNKS, 2, rows // CHUNKS, LANES), F32),
            pltpu.VMEM((2, CHUNKS, 2, rows // CHUNKS, LANES), F32),
            pltpu.VMEM((CHUNKS, 2, rows // CHUNKS, LANES), F32),
            pltpu.VMEM((CHUNKS, rows // CHUNKS, 12 * LANES), BF16),
            pltpu.VMEM((2, 8, 12 * LANES, span), HOT),
            pltpu.VMEM((2, 8, 4 * LANES, span), HOT),
            pltpu.VMEM((2, 8, span), jnp.int32),
            pltpu.VMEM((3, 2, 8, span), F32),
            pltpu.VMEM((2, 2, 8, span), F32),
            pltpu.VMEM((2, 2, 8, span), F32),
            pltpu.VMEM((8, LANES), F32),
            pltpu.VMEM((arcs, 8, LANES), F32),
            pltpu.VMEM((span, 32 * LANES), BF16),
            pltpu.VMEM((32, 32 * LANES), BF16),
            pltpu.VMEM((16, span), F32),
            pltpu.VMEM((comms, 16, span), F32),
            pltpu.VMEM((8, LANES), F32),
            pltpu.VMEM((ROW, 8, LANES), F32),
            pltpu.VMEM((8, LANES), F32),
            pltpu.VMEM((arcs // ROW, 8, LANES), F32),
            dma((2, SWEEPS, CHUNKS)),
            dma((2, SWEEPS, CHUNKS)),
            dma,
            dma,
            dma((2, ROW)),
            dma((2, ROW)),
            dma((2, arcs // ROW)),
            dma((2, arcs // ROW)),
            dma((7,)),
            dma((7,)),
        ],
        compiler_params=pltpu.CompilerParams(
            collective_id=0, has_side_effects=True, vmem_limit_bytes=63 * 1024 * 1024 - 65536
        ),
    )(
        prev_dist, source_node.reshape(1, rows), arc_tail, base_cost, arc_price, capacity,
        path_arcs, demand,
    )


def solution(mesh):
    in_specs = (
        P("comm", "arc"),
        P("comm"),
        P(None, "arc"),
        P(None, "arc"),
        P(None, "arc"),
        P(None, "arc"),
        P(("comm", "arc"), None),
        P(("comm", "arc")),
    )
    out_specs = (P("comm", "arc"), P(None, "arc"))
    return jax.shard_map(shards, mesh=mesh, in_specs=in_specs, out_specs=out_specs, check_vma=False)
```

```python
import functools

import jax
import jax.numpy as jnp
from jax import lax
from jax.experimental import pallas as pl
from jax.experimental.pallas import tpu as pltpu
from jax.sharding import PartitionSpec as P

SWEEPS = 8
CHUNKS = 1

LANES = 128
MESH = pl.DeviceIdType.MESH
F32 = jnp.float32
BF16 = jnp.bfloat16
HOT = jnp.float8_e4m3fn
ROW = 8

step_size = 0.25
eps_value = 1e-06


def parts(x):
    high = x.astype(BF16)
    return high, (x - high.astype(F32)).astype(BF16)


def kernel(
    arcs, comms, nodes,
    dist_hbm, source_hbm, tail_hbm, cost_hbm, price_hbm, cap_hbm, path_hbm, demand_ref,
    dist_out, price_out,
    dist_ref, source_ref, tail_ref, cost_ref, price_ref, cap_ref, path_ref, fetch_sem,
    own, reduced, beside, across, missing, best, lhs, hot, seen, rel, weight, tell, told,
    pay, routes, ends, picks, flow, flows, square, squares, square_sum, square_sums,
    near_send, near_recv, tell_send, tell_recv, row_send, row_recv, col_send, col_recv, flow_send, flow_recv,
):
    me = lax.axis_index("arc")
    group = lax.axis_index("comm")
    span = 2 * LANES
    rows = LANES // CHUNKS
    first = me * span
    after = lax.rem(me + 1, arcs)
    before = lax.rem(me + arcs - 1, arcs)

    barrier = pltpu.get_barrier_semaphore()
    fetches = [
        pltpu.make_async_copy(there, here, fetch_sem.at[k])
        for k, (there, here) in enumerate(
            (
                (tail_hbm, tail_ref),
                (cost_hbm, cost_ref),
                (price_hbm, price_ref),
                (source_hbm, source_ref),
                (dist_hbm, dist_ref),
                (path_hbm, path_ref),
                (cap_hbm, cap_ref),
            )
        )
    ]
    for fetch in fetches:
        fetch.start()

    core = lax.rem(me, 2)
    partner = me + 1 - 2 * core
    other = lax.rem(me + arcs - 1 + 2 * core, arcs)
    line = me // ROW
    place = lax.rem(me, ROW)
    lines = arcs // ROW

    def row_peer(step):
        return line * ROW + lax.rem(place + step, ROW)

    def col_peer(step):
        return lax.rem(line + step, lines) * ROW + place

    def ring(step):
        return lax.rem(group + comms + step, comms)

    greeted = [("arc", row_peer(step)) for step in range(1, ROW)]
    greeted += [("arc", col_peer(step)) for step in range(1, lines)]
    greeted += [("arc", after), ("arc", before)]
    greeted += [("comm", ring(step)) for step in (1, 2, -1, -2)]
    for axis, peer in greeted:
        pl.semaphore_signal(barrier, inc=1, device_id={axis: peer}, device_id_type=MESH)

    for fetch in fetches:
        fetch.wait()

    source = jnp.broadcast_to(source_ref[...], (LANES, LANES)).T
    lane = lax.broadcasted_iota(jnp.int32, (LANES, LANES), 1)
    for b in range(2):
        block = dist_ref[:, b * LANES : (b + 1) * LANES]
        block = jnp.where(source == lane + (first + b * LANES), F32(0.0), block)
        for c in range(CHUNKS):
            own[0, c, b] = block[c * rows : (c + 1) * rows]

    pay[0:4, :] = path_ref[...].astype(F32)
    for r in range(4):
        pay[4 + r : 5 + r, :] = jnp.full((1, LANES), demand_ref[r], F32)

    arc_weight = cost_ref[...] + price_ref[...]
    shifted = tail_ref[...] - (first - span)
    shifted = jnp.where(shifted < 0, shifted + nodes, shifted)
    shifted = jnp.where(shifted >= nodes, shifted - nodes, shifted)
    for h in range(2):
        cols = slice(h * LANES, (h + 1) * LANES)
        pair = jnp.concatenate([shifted[0:8, cols], shifted[8:16, cols]], axis=1)
        cost = jnp.concatenate([arc_weight[0:8, cols], arc_weight[8:16, cols]], axis=1)
        rel[h] = pair
        at = pair // LANES
        inside = (at == 2) | (at == 3)
        low = at < 2
        toward = jnp.where(low, core, 1 - core) == 1
        weight[0, h] = jnp.where(inside, cost, jnp.inf)
        weight[1, h] = jnp.where(inside | ~toward, jnp.inf, cost)
        weight[2, h] = jnp.where(inside | toward, jnp.inf, cost)
        tell[0, h] = pair.astype(F32)
        tell[1, h] = weight[2, h]

    row = lax.broadcasted_iota(jnp.int32, (LANES, span), 0)

    def fill(target, h, t, k, want, at):
        one = jnp.where(want - at * LANES == row, F32(1.0), F32(0.0)).astype(HOT)
        target[h, t, k * span : k * span + LANES, :] = one
        target[h, t, k * span + LANES : (k + 1) * span, :] = one

    @pl.loop(0, 8)
    def _(t):
        for h in range(2):
            want = jnp.broadcast_to(rel[h, pl.ds(t, 1), :], (LANES, span))
            for k, at in enumerate(
                (
                    2 + core,
                    3 - core,
                    4 * (1 - core) + core,
                    4 * (1 - core) + 1 - core,
                    4 * core + 1 - core,
                    4 * core + core,
                )
            ):
                fill(hot, h, t, k, want, at)

    for k in range(2):
        for c in range(CHUNKS):
            for b in range(2):
                missing[k, c, b] = jnp.full((rows, LANES), jnp.inf, F32)

    pl.semaphore_wait(barrier, len(greeted))

    def to_partner(sweep, c):
        return pltpu.make_async_remote_copy(
            src_ref=own.at[sweep, c],
            dst_ref=beside.at[sweep, c],
            send_sem=near_send.at[0, sweep, c],
            recv_sem=near_recv.at[0, sweep, c],
            device_id={"arc": partner},
            device_id_type=MESH,
        )

    def to_other(sweep, c, source_at):
        return pltpu.make_async_remote_copy(
            src_ref=source_at,
            dst_ref=across.at[sweep, c],
            send_sem=near_send.at[1, sweep, c],
            recv_sem=near_recv.at[1, sweep, c],
            device_id={"arc": other},
            device_id_type=MESH,
        )

    arcs_told = pltpu.make_async_remote_copy(
        src_ref=tell,
        dst_ref=told,
        send_sem=tell_send,
        recv_sem=tell_recv,
        device_id={"arc": other},
        device_id_type=MESH,
    )

    def row_copies(kind, source_at, target_at):
        return [
            pltpu.make_async_remote_copy(
                src_ref=source_at,
                dst_ref=target_at,
                send_sem=row_send.at[kind, step],
                recv_sem=row_recv.at[kind, step],
                device_id={"arc": row_peer(step)},
                device_id_type=MESH,
            )
            for step in range(1, ROW)
        ]

    def col_copies(kind, source_at, target_at):
        return [
            pltpu.make_async_remote_copy(
                src_ref=source_at,
                dst_ref=target_at,
                send_sem=col_send.at[kind, step],
                recv_sem=col_recv.at[kind, step],
                device_id={"arc": col_peer(step)},
                device_id_type=MESH,
            )
            for step in range(1, lines)
        ]

    def flow_copies(moves):
        return [
            pltpu.make_async_remote_copy(
                src_ref=flow if of is None else flows.at[ring(of)],
                dst_ref=flows.at[ring(0 if of is None else of)],
                send_sem=flow_send.at[k],
                recv_sem=flow_recv.at[k],
                device_id={"comm": ring(step)},
                device_id_type=MESH,
            )
            for k, of, step in moves
        ]

    mine = routes.at[pl.ds(pl.multiple_of(line * ROW, ROW), ROW)]
    row_pay = row_copies(0, pay, routes.at[me])
    col_pay = col_copies(0, mine, mine)
    near_flow = flow_copies([(0, None, 1), (1, None, 2), (2, None, -1), (3, None, -2)])
    far_flow = flow_copies([(4, 1, -2), (5, 2, -2), (6, -1, 2)])
    row_square = row_copies(1, square, squares.at[place])
    col_square = col_copies(1, square_sum, square_sums.at[line])

    def start(copies):
        for copy in copies:
            copy.start()

    def finish(copies):
        for copy in copies:
            copy.wait_send()
        for copy in copies:
            copy.wait_recv()

    def least(c, start, width, table, costs, best_dist):
        for t in range(8):
            found = jnp.dot(
                lhs[c, :, start : start + width], table(t), preferred_element_type=F32
            )
            found = found + costs(t)
            best_dist = jnp.minimum(best_dist, jnp.minimum(found[:, :LANES], found[:, LANES:]))
        return best_dist

    def phase(p, c, h, width, best_dist):
        start = p * 512
        return least(
            c, start, width,
            lambda t: hot[h, t, start : start + width, :],
            lambda t: weight[p, h, t : t + 1, :],
            best_dist,
        )

    def given(c, h, width):
        return least(
            c, 0, width,
            lambda t: seen[h, t, :width, :],
            lambda t: told[1, h, t : t + 1, :],
            jnp.full((rows, LANES), jnp.inf, F32),
        )

    def learn():
        arcs_told.wait_recv()

        @pl.loop(0, 8)
        def _(t):
            for h in range(2):
                want = told[0, h, pl.ds(t, 1), :].astype(jnp.int32)
                want = jnp.broadcast_to(want, (LANES, span))
                for k in range(2):
                    at = 4 * (1 - core) + (core if k == 0 else 1 - core)
                    fill(seen, h, t, k, want, at)

    def put(c, place, block):
        high, low = parts(block)
        lhs[c, :, place * span : place * span + LANES] = high
        lhs[c, :, place * span + LANES : (place + 1) * span] = low

    def count_line(step):
        node_row = lax.broadcasted_iota(jnp.int32, (span, LANES), 0)
        slot_row = lax.broadcasted_iota(jnp.int32, (16, LANES), 0)
        base = lax.rem(line + step, lines) * ROW
        for i in range(ROW):
            for r in range(4):
                at = slice((i * 4 + r) * LANES, (i * 4 + r + 1) * LANES)
                ids = routes[base + i, r : r + 1, :].astype(jnp.int32)
                amount = routes[base + i, 4 + r : 5 + r, :]
                node = jnp.broadcast_to((ids & (nodes - 1)) - first, (span, LANES))
                hop_slot = jnp.broadcast_to(ids // nodes, (16, LANES))
                ends[:, at] = jnp.where(node == node_row, F32(1.0), F32(0.0)).astype(HOT)
                given = jnp.where(hop_slot == slot_row, amount, F32(0.0))
                high, low = parts(given)
                picks[0:16, at] = high
                picks[16:32, at] = low
        both = lax.dot_general(
            picks[...], ends[...], (((1,), (1,)), ((), ())), preferred_element_type=F32
        )
        return both[0:16] + both[16:32]

    def flow_step(t):
        if t == 0:
            finish(row_pay)
            routes[me] = pay[...]
            start(col_pay)
        if t == 1:
            flow[...] = count_line(0)
        if t == 2:
            finish(col_pay)

            @pl.loop(1, 3)
            def _(step):
                flow[...] += count_line(step)
        if t == 3:
            flow[...] += count_line(3)
            flows[group] = flow[...]
            start(near_flow)
        if t == 4:
            finish(near_flow)
            start(far_flow)
        if t == 5:
            finish(far_flow)
            total = flows[0]
            for z in range(1, comms):
                total = total + flows[z]
            gradient = total - cap_ref[...]
            flow[...] = gradient
            sq = gradient * gradient
            square[...] = (sq[0:8, :LANES] + sq[8:16, :LANES]) + (sq[0:8, LANES:] + sq[8:16, LANES:])
            start(row_square)
        if t == 6:
            finish(row_square)
            squares[place] = square[...]
            total = squares[0]
            for a in range(1, ROW):
                total = total + squares[a]
            square_sum[...] = total
            start(col_square)
        if t == 7:
            finish(col_square)
            square_sums[line] = square_sum[...]
            total = square_sums[0]
            for a in range(1, lines):
                total = total + square_sums[a]
            whole = jnp.sum(total, axis=(0, 1), keepdims=True)
            root = jnp.sqrt(whole / F32(16 * nodes) + F32(eps_value))
            price_out[...] = jnp.maximum(
                price_ref[...] + F32(step_size) * flow[...] / root, F32(0.0)
            )

    for c in range(CHUNKS):
        to_other(0, c, own.at[0, c]).start()
        to_partner(0, c).start()
    arcs_told.start()
    start(row_pay)

    @pl.loop(0, SWEEPS)
    def _(sweep):
        slot = lax.rem(sweep, 2)
        for c in range(CHUNKS):
            for k, b in enumerate((core, 1 - core)):
                put(c, k, own[sweep, c, b])
            for h in range(2):
                best[c, h] = phase(0, c, h, 512, own[sweep, c, h])

        @pl.when(sweep > 0)
        def _():
            for c in range(CHUNKS):
                for h, width in ((1 - core, 512), (core, 256)):
                    missing[slot, c, h] = given(c, h, width)

        for c in range(CHUNKS):
            to_partner(sweep, c).wait_recv()
            for k, b in enumerate((core, 1 - core)):
                put(c, 2 + k, beside[sweep, c, b])
            for h, width in ((1 - core, 512), (core, 256)):
                reduced[sweep, c, h] = phase(1, c, h, width, best[c, h])

            @pl.when(sweep < SWEEPS - 1)
            def _():
                to_other(sweep + 1, c, reduced.at[sweep, c]).start()

        @pl.when(sweep == 0)
        def _():
            learn()
            for c in range(CHUNKS):
                for h, width in ((1 - core, 512), (core, 256)):
                    missing[slot, c, h] = given(c, h, width)

        for t in range(SWEEPS):
            pl.when(sweep == t)(functools.partial(flow_step, t))
        for c in range(CHUNKS):
            to_other(sweep, c, own.at[0, c]).wait_recv()
            for k, b in enumerate((1 - core, core)):
                put(c, 4 + k, jnp.minimum(across[sweep, c, b], missing[1 - slot, c, b]))
            for h, width in ((core, 512), (1 - core, 256)):
                own[sweep + 1, c, h] = phase(2, c, h, width, reduced[sweep, c, h])

            @pl.when(sweep < SWEEPS - 1)
            def _():
                to_partner(sweep + 1, c).start()

    for c in range(CHUNKS):
        for b in range(2):
            dist_out[c * rows : (c + 1) * rows, b * LANES : (b + 1) * LANES] = own[SWEEPS, c, b]

    arcs_told.wait_send()

    @pl.loop(0, SWEEPS)
    def _(sweep):
        for c in range(CHUNKS):
            to_partner(sweep, c).wait_send()
            to_other(sweep, c, own.at[0, c]).wait_send()


def shards(prev_dist, source_node, arc_tail, base_cost, arc_price, capacity, path_arcs, demand):
    arcs = lax.axis_size("arc")
    comms = lax.axis_size("comm")
    rows, span = prev_dist.shape
    vmem = pl.BlockSpec(memory_space=pltpu.VMEM)
    smem = pl.BlockSpec(memory_space=pltpu.SMEM)
    dma = pltpu.SemaphoreType.DMA
    return pl.pallas_call(
        functools.partial(kernel, arcs, comms, arcs * span),
        out_shape=(
            pltpu.VMEM(prev_dist.shape, F32),
            pltpu.VMEM(arc_price.shape, F32),
        ),
        in_specs=[pl.BlockSpec(memory_space=pltpu.HBM)] * 7 + [smem],
        out_specs=(vmem, vmem),
        scratch_shapes=[
            pltpu.VMEM(prev_dist.shape, F32),
            pltpu.VMEM((1, rows), jnp.int32),
            pltpu.VMEM(arc_tail.shape, jnp.int32),
            pltpu.VMEM(arc_price.shape, F32),
            pltpu.VMEM(arc_price.shape, F32),
            pltpu.VMEM(arc_price.shape, F32),
            pltpu.VMEM(path_arcs.shape, jnp.int32),
            dma((7,)),
            pltpu.VMEM((SWEEPS + 1, CHUNKS, 2, rows // CHUNKS, LANES), F32),
            pltpu.VMEM((SWEEPS, CHUNKS, 2, rows // CHUNKS, LANES), F32),
            pltpu.VMEM((SWEEPS, CHUNKS, 2, rows // CHUNKS, LANES), F32),
            pltpu.VMEM((SWEEPS, CHUNKS, 2, rows // CHUNKS, LANES), F32),
            pltpu.VMEM((2, CHUNKS, 2, rows // CHUNKS, LANES), F32),
            pltpu.VMEM((CHUNKS, 2, rows // CHUNKS, LANES), F32),
            pltpu.VMEM((CHUNKS, rows // CHUNKS, 12 * LANES), BF16),
            pltpu.VMEM((2, 8, 12 * LANES, span), HOT),
            pltpu.VMEM((2, 8, 4 * LANES, span), HOT),
            pltpu.VMEM((2, 8, span), jnp.int32),
            pltpu.VMEM((3, 2, 8, span), F32),
            pltpu.VMEM((2, 2, 8, span), F32),
            pltpu.VMEM((2, 2, 8, span), F32),
            pltpu.VMEM((8, LANES), F32),
            pltpu.VMEM((arcs, 8, LANES), F32),
            pltpu.VMEM((span, 32 * LANES), HOT),
            pltpu.VMEM((32, 32 * LANES), BF16),
            pltpu.VMEM((16, span), F32),
            pltpu.VMEM((comms, 16, span), F32),
            pltpu.VMEM((8, LANES), F32),
            pltpu.VMEM((ROW, 8, LANES), F32),
            pltpu.VMEM((8, LANES), F32),
            pltpu.VMEM((arcs // ROW, 8, LANES), F32),
            dma((2, SWEEPS, CHUNKS)),
            dma((2, SWEEPS, CHUNKS)),
            dma,
            dma,
            dma((2, ROW)),
            dma((2, ROW)),
            dma((2, arcs // ROW)),
            dma((2, arcs // ROW)),
            dma((7,)),
            dma((7,)),
        ],
        compiler_params=pltpu.CompilerParams(
            collective_id=0, has_side_effects=True, vmem_limit_bytes=63 * 1024 * 1024 - 65536
        ),
    )(
        prev_dist, source_node.reshape(1, rows), arc_tail, base_cost, arc_price, capacity,
        path_arcs, demand,
    )


def solution(mesh):
    in_specs = (
        P("comm", "arc"),
        P("comm"),
        P(None, "arc"),
        P(None, "arc"),
        P(None, "arc"),
        P(None, "arc"),
        P(("comm", "arc"), None),
        P(("comm", "arc")),
    )
    out_specs = (P("comm", "arc"), P(None, "arc"))
    return jax.shard_map(shards, mesh=mesh, in_specs=in_specs, out_specs=out_specs, check_vma=False)
```

```python
import functools

import jax
import jax.numpy as jnp
from jax import lax
from jax.experimental import pallas as pl
from jax.experimental.pallas import tpu as pltpu
from jax.sharding import PartitionSpec as P

SWEEPS = 8
CHUNKS = 1

LANES = 128
MESH = pl.DeviceIdType.MESH
F32 = jnp.float32
BF16 = jnp.bfloat16
HOT = jnp.float8_e4m3fn
ROW = 8

step_size = 0.25
eps_value = 1e-06


def parts(x):
    high = x.astype(BF16)
    return high, (x - high.astype(F32)).astype(BF16)


def kernel(
    arcs, comms, nodes,
    dist_hbm, source_hbm, tail_hbm, cost_hbm, price_hbm, cap_hbm, path_hbm, demand_ref,
    dist_out, price_out,
    dist_ref, source_ref, tail_ref, cost_ref, price_ref, cap_ref, path_ref, fetch_sem,
    own, reduced, beside, across, missing, best, lhs, hot, seen, rel, weight, tell, told,
    pay, routes, ends, picks, flow, flows, square, squares, square_sum, square_sums,
    near_send, near_recv, tell_send, tell_recv, row_send, row_recv, col_send, col_recv, flow_send, flow_recv,
):
    me = lax.axis_index("arc")
    group = lax.axis_index("comm")
    span = 2 * LANES
    rows = LANES // CHUNKS
    first = me * span
    after = lax.rem(me + 1, arcs)
    before = lax.rem(me + arcs - 1, arcs)

    barrier = pltpu.get_barrier_semaphore()
    fetches = [
        pltpu.make_async_copy(there, here, fetch_sem.at[k])
        for k, (there, here) in enumerate(
            (
                (tail_hbm, tail_ref),
                (cost_hbm, cost_ref),
                (price_hbm, price_ref),
                (source_hbm, source_ref),
                (dist_hbm, dist_ref),
                (path_hbm, path_ref),
                (cap_hbm, cap_ref),
            )
        )
    ]
    for fetch in fetches:
        fetch.start()

    core = lax.rem(me, 2)
    partner = me + 1 - 2 * core
    other = lax.rem(me + arcs - 1 + 2 * core, arcs)
    line = me // ROW
    place = lax.rem(me, ROW)
    lines = arcs // ROW

    def row_peer(step):
        return line * ROW + lax.rem(place + step, ROW)

    def col_peer(step):
        return lax.rem(line + step, lines) * ROW + place

    def ring(step):
        return lax.rem(group + comms + step, comms)

    greeted = [("arc", row_peer(step)) for step in range(1, ROW)]
    greeted += [("arc", col_peer(step)) for step in range(1, lines)]
    greeted += [("arc", after), ("arc", before)]
    greeted += [("comm", ring(step)) for step in (1, 2, -1, -2)]
    for axis, peer in greeted:
        pl.semaphore_signal(barrier, inc=1, device_id={axis: peer}, device_id_type=MESH)

    for fetch in fetches:
        fetch.wait()

    source = jnp.broadcast_to(source_ref[...], (LANES, LANES)).T
    lane = lax.broadcasted_iota(jnp.int32, (LANES, LANES), 1)
    for b in range(2):
        block = dist_ref[:, b * LANES : (b + 1) * LANES]
        block = jnp.where(source == lane + (first + b * LANES), F32(0.0), block)
        for c in range(CHUNKS):
            own[0, c, b] = block[c * rows : (c + 1) * rows]

    pay[0:4, :] = path_ref[...].astype(F32)
    for r in range(4):
        pay[4 + r : 5 + r, :] = jnp.full((1, LANES), demand_ref[r], F32)

    arc_weight = cost_ref[...] + price_ref[...]
    shifted = tail_ref[...] - (first - span)
    shifted = jnp.where(shifted < 0, shifted + nodes, shifted)
    shifted = jnp.where(shifted >= nodes, shifted - nodes, shifted)
    for h in range(2):
        cols = slice(h * LANES, (h + 1) * LANES)
        pair = jnp.concatenate([shifted[0:8, cols], shifted[8:16, cols]], axis=1)
        cost = jnp.concatenate([arc_weight[0:8, cols], arc_weight[8:16, cols]], axis=1)
        rel[h] = pair
        at = pair // LANES
        inside = (at == 2) | (at == 3)
        low = at < 2
        toward = jnp.where(low, core, 1 - core) == 1
        weight[0, h] = jnp.where(inside, cost, jnp.inf)
        weight[1, h] = jnp.where(inside | ~toward, jnp.inf, cost)
        weight[2, h] = jnp.where(inside | toward, jnp.inf, cost)
        tell[0, h] = pair.astype(F32)
        tell[1, h] = weight[2, h]

    row = lax.broadcasted_iota(jnp.int32, (LANES, span), 0)

    def fill(target, h, t, k, want, at):
        one = jnp.where(want - at * LANES == row, F32(1.0), F32(0.0)).astype(HOT)
        target[h, t, k * span : k * span + LANES, :] = one
        target[h, t, k * span + LANES : (k + 1) * span, :] = one

    pl.semaphore_wait(barrier, len(greeted))

    def to_partner(sweep, c):
        return pltpu.make_async_remote_copy(
            src_ref=own.at[sweep, c],
            dst_ref=beside.at[sweep, c],
            send_sem=near_send.at[0, sweep, c],
            recv_sem=near_recv.at[0, sweep, c],
            device_id={"arc": partner},
            device_id_type=MESH,
        )

    def to_other(sweep, c, source_at):
        return pltpu.make_async_remote_copy(
            src_ref=source_at,
            dst_ref=across.at[sweep, c],
            send_sem=near_send.at[1, sweep, c],
            recv_sem=near_recv.at[1, sweep, c],
            device_id={"arc": other},
            device_id_type=MESH,
        )

    arcs_told = pltpu.make_async_remote_copy(
        src_ref=tell,
        dst_ref=told,
        send_sem=tell_send,
        recv_sem=tell_recv,
        device_id={"arc": other},
        device_id_type=MESH,
    )

    def row_copies(kind, source_at, target_at):
        return [
            pltpu.make_async_remote_copy(
                src_ref=source_at,
                dst_ref=target_at,
                send_sem=row_send.at[kind, step],
                recv_sem=row_recv.at[kind, step],
                device_id={"arc": row_peer(step)},
                device_id_type=MESH,
            )
            for step in range(1, ROW)
        ]

    def col_copies(kind, source_at, target_at):
        return [
            pltpu.make_async_remote_copy(
                src_ref=source_at,
                dst_ref=target_at,
                send_sem=col_send.at[kind, step],
                recv_sem=col_recv.at[kind, step],
                device_id={"arc": col_peer(step)},
                device_id_type=MESH,
            )
            for step in range(1, lines)
        ]

    def flow_copies(moves):
        return [
            pltpu.make_async_remote_copy(
                src_ref=flow if of is None else flows.at[ring(of)],
                dst_ref=flows.at[ring(0 if of is None else of)],
                send_sem=flow_send.at[k],
                recv_sem=flow_recv.at[k],
                device_id={"comm": ring(step)},
                device_id_type=MESH,
            )
            for k, of, step in moves
        ]

    mine = routes.at[pl.ds(pl.multiple_of(line * ROW, ROW), ROW)]
    row_pay = row_copies(0, pay, routes.at[me])
    col_pay = col_copies(0, mine, mine)
    near_flow = flow_copies([(0, None, 1), (1, None, 2), (2, None, -1), (3, None, -2)])
    far_flow = flow_copies([(4, 1, -2), (5, 2, -2), (6, -1, 2)])
    row_square = row_copies(1, square, squares.at[place])
    col_square = col_copies(1, square_sum, square_sums.at[line])

    def start(copies):
        for copy in copies:
            copy.start()

    def finish(copies):
        for copy in copies:
            copy.wait_send()
        for copy in copies:
            copy.wait_recv()

    def least(c, start, width, table, costs, best_dist):
        for t in range(8):
            found = jnp.dot(
                lhs[c, :, start : start + width], table(t), preferred_element_type=F32
            )
            found = found + costs(t)
            best_dist = jnp.minimum(best_dist, jnp.minimum(found[:, :LANES], found[:, LANES:]))
        return best_dist

    def phase(p, c, h, width, best_dist):
        start = p * 512
        return least(
            c, start, width,
            lambda t: hot[h, t, start : start + width, :],
            lambda t: weight[p, h, t : t + 1, :],
            best_dist,
        )

    def given(c, h, width):
        return least(
            c, 0, width,
            lambda t: seen[h, t, :width, :],
            lambda t: told[1, h, t : t + 1, :],
            jnp.full((rows, LANES), jnp.inf, F32),
        )

    def learn():
        arcs_told.wait_recv()

        @pl.loop(0, 8)
        def _(t):
            for h in range(2):
                want = told[0, h, pl.ds(t, 1), :].astype(jnp.int32)
                want = jnp.broadcast_to(want, (LANES, span))
                for k in range(2):
                    at = 4 * (1 - core) + (core if k == 0 else 1 - core)
                    fill(seen, h, t, k, want, at)

    def put(c, place, block):
        high, low = parts(block)
        lhs[c, :, place * span : place * span + LANES] = high
        lhs[c, :, place * span + LANES : (place + 1) * span] = low

    def count_line(step):
        node_row = lax.broadcasted_iota(jnp.int32, (LANES, LANES), 0)
        place_row = lax.broadcasted_iota(jnp.int32, (32, LANES), 0)
        base = lax.rem(line + step, lines) * ROW
        for i in range(ROW):
            for r in range(4):
                at = slice((i * 4 + r) * LANES, (i * 4 + r + 1) * LANES)
                ids = routes[base + i, r : r + 1, :].astype(jnp.int32)
                amount = routes[base + i, 4 + r : 5 + r, :]
                node = (ids & (nodes - 1)) - first
                here = (node >= 0) & (node < span)
                spot = jnp.where(here, (node // LANES) * 16 + ids // nodes, -1)
                lane_of = jnp.broadcast_to(node & (LANES - 1), (LANES, LANES))
                ends[:, at] = jnp.where(lane_of == node_row, F32(1.0), F32(0.0)).astype(HOT)
                carried = jnp.where(
                    jnp.broadcast_to(spot, (32, LANES)) == place_row, amount, F32(0.0)
                )
                high, low = parts(carried)
                picks[0:32, at] = high
                picks[32:64, at] = low
        both = lax.dot_general(
            picks[...], ends[...], (((1,), (1,)), ((), ())), preferred_element_type=F32
        )
        both = both[0:32] + both[32:64]
        return jnp.concatenate([both[0:16], both[16:32]], axis=1)

    def flow_step(t):
        if t == 0:
            finish(row_pay)
            routes[me] = pay[...]
            start(col_pay)
            flow[...] = count_line(0)
        if t == 1:
            finish(col_pay)

            @pl.loop(1, lines)
            def _(step):
                flow[...] += count_line(step)

            flows[group] = flow[...]
            start(near_flow)
        if t == 3:
            finish(near_flow)
            start(far_flow)
        if t == 5:
            finish(far_flow)
            total = flows[0]
            for z in range(1, comms):
                total = total + flows[z]
            gradient = total - cap_ref[...]
            flow[...] = gradient
            sq = gradient * gradient
            square[...] = (sq[0:8, :LANES] + sq[8:16, :LANES]) + (sq[0:8, LANES:] + sq[8:16, LANES:])
            start(row_square)
        if t == 6:
            finish(row_square)
            squares[place] = square[...]
            total = squares[0]
            for a in range(1, ROW):
                total = total + squares[a]
            square_sum[...] = total
            start(col_square)
        if t == 7:
            finish(col_square)
            square_sums[line] = square_sum[...]
            total = square_sums[0]
            for a in range(1, lines):
                total = total + square_sums[a]
            whole = jnp.sum(total, axis=(0, 1), keepdims=True)
            root = jnp.sqrt(whole / F32(16 * nodes) + F32(eps_value))
            price_out[...] = jnp.maximum(
                price_ref[...] + F32(step_size) * flow[...] / root, F32(0.0)
            )

    for c in range(CHUNKS):
        to_other(0, c, own.at[0, c]).start()
        to_partner(0, c).start()
    arcs_told.start()
    start(row_pay)

    @pl.loop(0, 8)
    def _(t):
        for h in range(2):
            want = jnp.broadcast_to(rel[h, pl.ds(t, 1), :], (LANES, span))
            for k, at in enumerate(
                (
                    2 + core,
                    3 - core,
                    4 * (1 - core) + core,
                    4 * (1 - core) + 1 - core,
                    4 * core + 1 - core,
                    4 * core + core,
                )
            ):
                fill(hot, h, t, k, want, at)

    for k in range(2):
        for c in range(CHUNKS):
            for b in range(2):
                missing[k, c, b] = jnp.full((rows, LANES), jnp.inf, F32)

    @pl.loop(0, SWEEPS)
    def _(sweep):
        slot = lax.rem(sweep, 2)
        for c in range(CHUNKS):
            for k, b in enumerate((core, 1 - core)):
                put(c, k, own[sweep, c, b])
            for h in range(2):
                best[c, h] = phase(0, c, h, 512, own[sweep, c, h])

        @pl.when((sweep > 0) & (sweep < SWEEPS - 1))
        def _():
            for c in range(CHUNKS):
                for h, width in ((1 - core, 512), (core, 256)):
                    missing[slot, c, h] = given(c, h, width)

        for c in range(CHUNKS):
            to_partner(sweep, c).wait_recv()
            for k, b in enumerate((core, 1 - core)):
                put(c, 2 + k, beside[sweep, c, b])
            for h, width in ((1 - core, 512), (core, 256)):
                reduced[sweep, c, h] = phase(1, c, h, width, best[c, h])

            @pl.when(sweep < SWEEPS - 1)
            def _():
                to_other(sweep + 1, c, reduced.at[sweep, c]).start()

        @pl.when(sweep == 0)
        def _():
            learn()
            for c in range(CHUNKS):
                for h, width in ((1 - core, 512), (core, 256)):
                    missing[slot, c, h] = given(c, h, width)

        for t in range(SWEEPS):
            pl.when(sweep == t)(functools.partial(flow_step, t))
        for c in range(CHUNKS):
            to_other(sweep, c, own.at[0, c]).wait_recv()
            for k, b in enumerate((1 - core, core)):
                put(c, 4 + k, jnp.minimum(across[sweep, c, b], missing[1 - slot, c, b]))
            for h, width in ((core, 512), (1 - core, 256)):
                own[sweep + 1, c, h] = phase(2, c, h, width, reduced[sweep, c, h])

            @pl.when(sweep < SWEEPS - 1)
            def _():
                to_partner(sweep + 1, c).start()

    for c in range(CHUNKS):
        for b in range(2):
            dist_out[c * rows : (c + 1) * rows, b * LANES : (b + 1) * LANES] = own[SWEEPS, c, b]

    arcs_told.wait_send()

    @pl.loop(0, SWEEPS)
    def _(sweep):
        for c in range(CHUNKS):
            to_partner(sweep, c).wait_send()
            to_other(sweep, c, own.at[0, c]).wait_send()


def shards(prev_dist, source_node, arc_tail, base_cost, arc_price, capacity, path_arcs, demand):
    arcs = lax.axis_size("arc")
    comms = lax.axis_size("comm")
    rows, span = prev_dist.shape
    vmem = pl.BlockSpec(memory_space=pltpu.VMEM)
    smem = pl.BlockSpec(memory_space=pltpu.SMEM)
    dma = pltpu.SemaphoreType.DMA
    return pl.pallas_call(
        functools.partial(kernel, arcs, comms, arcs * span),
        out_shape=(
            pltpu.VMEM(prev_dist.shape, F32),
            pltpu.VMEM(arc_price.shape, F32),
        ),
        in_specs=[pl.BlockSpec(memory_space=pltpu.HBM)] * 7 + [smem],
        out_specs=(vmem, vmem),
        scratch_shapes=[
            pltpu.VMEM(prev_dist.shape, F32),
            pltpu.VMEM((1, rows), jnp.int32),
            pltpu.VMEM(arc_tail.shape, jnp.int32),
            pltpu.VMEM(arc_price.shape, F32),
            pltpu.VMEM(arc_price.shape, F32),
            pltpu.VMEM(arc_price.shape, F32),
            pltpu.VMEM(path_arcs.shape, jnp.int32),
            dma((7,)),
            pltpu.VMEM((SWEEPS + 1, CHUNKS, 2, rows // CHUNKS, LANES), F32),
            pltpu.VMEM((SWEEPS, CHUNKS, 2, rows // CHUNKS, LANES), F32),
            pltpu.VMEM((SWEEPS, CHUNKS, 2, rows // CHUNKS, LANES), F32),
            pltpu.VMEM((SWEEPS, CHUNKS, 2, rows // CHUNKS, LANES), F32),
            pltpu.VMEM((2, CHUNKS, 2, rows // CHUNKS, LANES), F32),
            pltpu.VMEM((CHUNKS, 2, rows // CHUNKS, LANES), F32),
            pltpu.VMEM((CHUNKS, rows // CHUNKS, 12 * LANES), BF16),
            pltpu.VMEM((2, 8, 12 * LANES, span), HOT),
            pltpu.VMEM((2, 8, 4 * LANES, span), HOT),
            pltpu.VMEM((2, 8, span), jnp.int32),
            pltpu.VMEM((3, 2, 8, span), F32),
            pltpu.VMEM((2, 2, 8, span), F32),
            pltpu.VMEM((2, 2, 8, span), F32),
            pltpu.VMEM((8, LANES), F32),
            pltpu.VMEM((arcs, 8, LANES), F32),
            pltpu.VMEM((LANES, 32 * LANES), HOT),
            pltpu.VMEM((64, 32 * LANES), BF16),
            pltpu.VMEM((16, span), F32),
            pltpu.VMEM((comms, 16, span), F32),
            pltpu.VMEM((8, LANES), F32),
            pltpu.VMEM((ROW, 8, LANES), F32),
            pltpu.VMEM((8, LANES), F32),
            pltpu.VMEM((arcs // ROW, 8, LANES), F32),
            dma((2, SWEEPS, CHUNKS)),
            dma((2, SWEEPS, CHUNKS)),
            dma,
            dma,
            dma((2, ROW)),
            dma((2, ROW)),
            dma((2, arcs // ROW)),
            dma((2, arcs // ROW)),
            dma((7,)),
            dma((7,)),
        ],
        compiler_params=pltpu.CompilerParams(
            collective_id=0, has_side_effects=True, vmem_limit_bytes=63 * 1024 * 1024 - 65536
        ),
    )(
        prev_dist, source_node.reshape(1, rows), arc_tail, base_cost, arc_price, capacity,
        path_arcs, demand,
    )


def solution(mesh):
    in_specs = (
        P("comm", "arc"),
        P("comm"),
        P(None, "arc"),
        P(None, "arc"),
        P(None, "arc"),
        P(None, "arc"),
        P(("comm", "arc"), None),
        P(("comm", "arc")),
    )
    out_specs = (P("comm", "arc"), P(None, "arc"))
    return jax.shard_map(shards, mesh=mesh, in_specs=in_specs, out_specs=out_specs, check_vma=False)
```

```python
import functools

import jax
import jax.numpy as jnp
from jax import lax
from jax.experimental import pallas as pl
from jax.experimental.pallas import tpu as pltpu
from jax.sharding import PartitionSpec as P

SWEEPS = 8
CHUNKS = 1

LANES = 128
MESH = pl.DeviceIdType.MESH
F32 = jnp.float32
BF16 = jnp.bfloat16
HOT = jnp.float8_e4m3fn
ROW = 8

step_size = 0.25
eps_value = 1e-06


def parts(x):
    high = x.astype(BF16)
    return high, (x - high.astype(F32)).astype(BF16)


def kernel(
    arcs, comms, nodes,
    dist_hbm, source_hbm, tail_hbm, cost_hbm, price_hbm, cap_hbm, path_hbm, demand_ref,
    dist_out, price_out,
    dist_ref, source_ref, tail_ref, cost_ref, price_ref, cap_ref, path_ref, fetch_sem,
    own, reduced, beside, across, missing, best, lhs, hot, seen, rel, weight, tell, told,
    pay, routes, ends, picks, flow, flows, square, squares, square_sum, square_sums,
    near_send, near_recv, tell_send, tell_recv, row_send, row_recv, col_send, col_recv, flow_send, flow_recv,
):
    me = lax.axis_index("arc")
    group = lax.axis_index("comm")
    span = 2 * LANES
    rows = LANES // CHUNKS
    first = me * span
    after = lax.rem(me + 1, arcs)
    before = lax.rem(me + arcs - 1, arcs)

    barrier = pltpu.get_barrier_semaphore()
    fetches = [
        pltpu.make_async_copy(there, here, fetch_sem.at[k])
        for k, (there, here) in enumerate(
            (
                (tail_hbm, tail_ref),
                (cost_hbm, cost_ref),
                (price_hbm, price_ref),
                (source_hbm, source_ref),
                (dist_hbm, dist_ref),
                (path_hbm, path_ref),
                (cap_hbm, cap_ref),
            )
        )
    ]
    for fetch in fetches:
        fetch.start()

    core = lax.rem(me, 2)
    partner = me + 1 - 2 * core
    other = lax.rem(me + arcs - 1 + 2 * core, arcs)
    line = me // ROW
    place = lax.rem(me, ROW)
    lines = arcs // ROW

    def row_peer(step):
        return line * ROW + lax.rem(place + step, ROW)

    def col_peer(step):
        return lax.rem(line + step, lines) * ROW + place

    def ring(step):
        return lax.rem(group + comms + step, comms)

    greeted = [("arc", row_peer(step)) for step in range(1, ROW)]
    greeted += [("arc", col_peer(step)) for step in range(1, lines)]
    greeted += [("arc", after), ("arc", before)]
    greeted += [("comm", ring(step)) for step in (1, 2, -1, -2)]
    for axis, peer in greeted:
        pl.semaphore_signal(barrier, inc=1, device_id={axis: peer}, device_id_type=MESH)

    for fetch in fetches:
        fetch.wait()

    source = jnp.broadcast_to(source_ref[...], (LANES, LANES)).T
    lane = lax.broadcasted_iota(jnp.int32, (LANES, LANES), 1)
    for b in range(2):
        block = dist_ref[:, b * LANES : (b + 1) * LANES]
        block = jnp.where(source == lane + (first + b * LANES), F32(0.0), block)
        for c in range(CHUNKS):
            own[0, c, b] = block[c * rows : (c + 1) * rows]

    pay[0:4, :] = path_ref[...].astype(F32)
    for r in range(4):
        pay[4 + r : 5 + r, :] = jnp.full((1, LANES), demand_ref[r], F32)

    arc_weight = cost_ref[...] + price_ref[...]
    shifted = tail_ref[...] - (first - span)
    shifted = jnp.where(shifted < 0, shifted + nodes, shifted)
    shifted = jnp.where(shifted >= nodes, shifted - nodes, shifted)
    for h in range(2):
        cols = slice(h * LANES, (h + 1) * LANES)
        pair = jnp.concatenate([shifted[0:8, cols], shifted[8:16, cols]], axis=1)
        cost = jnp.concatenate([arc_weight[0:8, cols], arc_weight[8:16, cols]], axis=1)
        rel[h] = pair
        at = pair // LANES
        inside = (at == 2) | (at == 3)
        low = at < 2
        toward = jnp.where(low, core, 1 - core) == 1
        weight[0, h] = jnp.where(inside, cost, jnp.inf)
        weight[1, h] = jnp.where(inside | ~toward, jnp.inf, cost)
        weight[2, h] = jnp.where(inside | toward, jnp.inf, cost)
        tell[0, h] = pair.astype(F32)
        tell[1, h] = weight[2, h]

    row = lax.broadcasted_iota(jnp.int32, (LANES, span), 0)

    def fill(target, h, t, k, want, at):
        one = jnp.where(want - at * LANES == row, F32(1.0), F32(0.0)).astype(HOT)
        target[h, t, k * span : k * span + LANES, :] = one
        target[h, t, k * span + LANES : (k + 1) * span, :] = one

    pl.semaphore_wait(barrier, len(greeted))

    def to_partner(sweep, c):
        return pltpu.make_async_remote_copy(
            src_ref=own.at[sweep, c],
            dst_ref=beside.at[sweep, c],
            send_sem=near_send.at[0, sweep, c],
            recv_sem=near_recv.at[0, sweep, c],
            device_id={"arc": partner},
            device_id_type=MESH,
        )

    def to_other(sweep, c, source_at):
        return pltpu.make_async_remote_copy(
            src_ref=source_at,
            dst_ref=across.at[sweep, c],
            send_sem=near_send.at[1, sweep, c],
            recv_sem=near_recv.at[1, sweep, c],
            device_id={"arc": other},
            device_id_type=MESH,
        )

    arcs_told = pltpu.make_async_remote_copy(
        src_ref=tell,
        dst_ref=told,
        send_sem=tell_send,
        recv_sem=tell_recv,
        device_id={"arc": other},
        device_id_type=MESH,
    )

    def row_copies(kind, source_at, target_at):
        return [
            pltpu.make_async_remote_copy(
                src_ref=source_at,
                dst_ref=target_at,
                send_sem=row_send.at[kind, step],
                recv_sem=row_recv.at[kind, step],
                device_id={"arc": row_peer(step)},
                device_id_type=MESH,
            )
            for step in range(1, ROW)
        ]

    def col_copies(kind, source_at, target_at):
        return [
            pltpu.make_async_remote_copy(
                src_ref=source_at,
                dst_ref=target_at,
                send_sem=col_send.at[kind, step],
                recv_sem=col_recv.at[kind, step],
                device_id={"arc": col_peer(step)},
                device_id_type=MESH,
            )
            for step in range(1, lines)
        ]

    def flow_copies(moves):
        return [
            pltpu.make_async_remote_copy(
                src_ref=flow if of is None else flows.at[ring(of)],
                dst_ref=flows.at[ring(0 if of is None else of)],
                send_sem=flow_send.at[k],
                recv_sem=flow_recv.at[k],
                device_id={"comm": ring(step)},
                device_id_type=MESH,
            )
            for k, of, step in moves
        ]

    mine = routes.at[pl.ds(pl.multiple_of(line * ROW, ROW), ROW)]
    row_pay = row_copies(0, pay, routes.at[me])
    col_pay = col_copies(0, mine, mine)
    near_flow = flow_copies([(0, None, 1), (1, None, 2), (2, None, -1), (3, None, -2)])
    far_flow = flow_copies([(4, 1, -2), (5, 2, -2), (6, -1, 2)])
    row_square = row_copies(1, square, squares.at[place])
    col_square = col_copies(1, square_sum, square_sums.at[line])

    def start(copies):
        for copy in copies:
            copy.start()

    def finish(copies):
        for copy in copies:
            copy.wait_send()
        for copy in copies:
            copy.wait_recv()

    def least(c, start, width, table, costs, best_dist):
        for t in range(8):
            found = jnp.dot(
                lhs[c, :, start : start + width], table(t), preferred_element_type=F32
            )
            found = found + costs(t)
            best_dist = jnp.minimum(best_dist, jnp.minimum(found[:, :LANES], found[:, LANES:]))
        return best_dist

    def phase(p, c, h, width, best_dist):
        start = p * 512
        return least(
            c, start, width,
            lambda t: hot[h, t, start : start + width, :],
            lambda t: weight[p, h, t : t + 1, :],
            best_dist,
        )

    def given(c, h, width):
        return least(
            c, 0, width,
            lambda t: seen[h, t, :width, :],
            lambda t: told[1, h, t : t + 1, :],
            jnp.full((rows, LANES), jnp.inf, F32),
        )

    def learn():
        arcs_told.wait_recv()

        @pl.loop(0, 8)
        def _(t):
            for h in range(2):
                want = told[0, h, pl.ds(t, 1), :].astype(jnp.int32)
                want = jnp.broadcast_to(want, (LANES, span))
                for k in range(2):
                    at = 4 * (1 - core) + (core if k == 0 else 1 - core)
                    fill(seen, h, t, k, want, at)

    def put(c, place, block):
        high, low = parts(block)
        lhs[c, :, place * span : place * span + LANES] = high
        lhs[c, :, place * span + LANES : (place + 1) * span] = low

    def count_line(step):
        node_row = lax.broadcasted_iota(jnp.int32, (LANES, LANES), 0)
        place_row = lax.broadcasted_iota(jnp.int32, (32, LANES), 0)
        base = lax.rem(line + step, lines) * ROW
        for i in range(ROW):
            for r in range(4):
                at = slice((i * 4 + r) * LANES, (i * 4 + r + 1) * LANES)
                ids = routes[base + i, r : r + 1, :].astype(jnp.int32)
                amount = routes[base + i, 4 + r : 5 + r, :]
                node = (ids & (nodes - 1)) - first
                here = (node >= 0) & (node < span)
                spot = jnp.where(here, (node // LANES) * 16 + ids // nodes, -1)
                lane_of = jnp.broadcast_to(node & (LANES - 1), (LANES, LANES))
                ends[:, at] = jnp.where(lane_of == node_row, F32(1.0), F32(0.0)).astype(HOT)
                carried = jnp.where(
                    jnp.broadcast_to(spot, (32, LANES)) == place_row, amount, F32(0.0)
                )
                high, low = parts(carried)
                picks[0:32, at] = high
                picks[32:64, at] = low
        both = lax.dot_general(
            picks[...], ends[...], (((1,), (1,)), ((), ())), preferred_element_type=F32
        )
        both = both[0:32] + both[32:64]
        return jnp.concatenate([both[0:16], both[16:32]], axis=1)

    def flow_step(t):
        if t == 0:
            finish(row_pay)
            routes[me] = pay[...]
            start(col_pay)
            flow[...] = count_line(0)
        if t == 1:
            finish(col_pay)
        if t in (1, 2, 3):
            flow[...] += count_line(t)
        if t == 3:
            flows[group] = flow[...]
            start(near_flow)
        if t == 4:
            finish(near_flow)
            start(far_flow)
        if t == 5:
            finish(far_flow)
            total = flows[0]
            for z in range(1, comms):
                total = total + flows[z]
            gradient = total - cap_ref[...]
            flow[...] = gradient
            sq = gradient * gradient
            square[...] = (sq[0:8, :LANES] + sq[8:16, :LANES]) + (sq[0:8, LANES:] + sq[8:16, LANES:])
            start(row_square)
        if t == 6:
            finish(row_square)
            squares[place] = square[...]
            total = squares[0]
            for a in range(1, ROW):
                total = total + squares[a]
            square_sum[...] = total
            start(col_square)
        if t == 7:
            finish(col_square)
            square_sums[line] = square_sum[...]
            total = square_sums[0]
            for a in range(1, lines):
                total = total + square_sums[a]
            whole = jnp.sum(total, axis=(0, 1), keepdims=True)
            root = jnp.sqrt(whole / F32(16 * nodes) + F32(eps_value))
            price_out[...] = jnp.maximum(
                price_ref[...] + F32(step_size) * flow[...] / root, F32(0.0)
            )

    for c in range(CHUNKS):
        to_other(0, c, own.at[0, c]).start()
        to_partner(0, c).start()
    arcs_told.start()
    start(row_pay)

    @pl.loop(0, 8)
    def _(t):
        for h in range(2):
            want = jnp.broadcast_to(rel[h, pl.ds(t, 1), :], (LANES, span))
            for k, at in enumerate(
                (
                    2 + core,
                    3 - core,
                    4 * (1 - core) + core,
                    4 * (1 - core) + 1 - core,
                    4 * core + 1 - core,
                    4 * core + core,
                )
            ):
                fill(hot, h, t, k, want, at)

    for k in range(2):
        for c in range(CHUNKS):
            for b in range(2):
                missing[k, c, b] = jnp.full((rows, LANES), jnp.inf, F32)

    @pl.loop(0, SWEEPS)
    def _(sweep):
        slot = lax.rem(sweep, 2)
        for c in range(CHUNKS):
            for k, b in enumerate((core, 1 - core)):
                put(c, k, own[sweep, c, b])
            for h in range(2):
                best[c, h] = phase(0, c, h, 512, own[sweep, c, h])

        @pl.when((sweep > 0) & (sweep < SWEEPS - 1))
        def _():
            for c in range(CHUNKS):
                for h, width in ((1 - core, 512), (core, 256)):
                    missing[slot, c, h] = given(c, h, width)

        for c in range(CHUNKS):
            to_partner(sweep, c).wait_recv()
            for k, b in enumerate((core, 1 - core)):
                put(c, 2 + k, beside[sweep, c, b])
            for h, width in ((1 - core, 512), (core, 256)):
                reduced[sweep, c, h] = phase(1, c, h, width, best[c, h])

            @pl.when(sweep < SWEEPS - 1)
            def _():
                to_other(sweep + 1, c, reduced.at[sweep, c]).start()

        @pl.when(sweep == 0)
        def _():
            learn()
            for c in range(CHUNKS):
                for h, width in ((1 - core, 512), (core, 256)):
                    missing[slot, c, h] = given(c, h, width)

        for t in range(SWEEPS):
            pl.when(sweep == t)(functools.partial(flow_step, t))
        for c in range(CHUNKS):
            to_other(sweep, c, own.at[0, c]).wait_recv()
            for k, b in enumerate((1 - core, core)):
                put(c, 4 + k, jnp.minimum(across[sweep, c, b], missing[1 - slot, c, b]))
            for h, width in ((core, 512), (1 - core, 256)):
                own[sweep + 1, c, h] = phase(2, c, h, width, reduced[sweep, c, h])

            @pl.when(sweep < SWEEPS - 1)
            def _():
                to_partner(sweep + 1, c).start()

    for c in range(CHUNKS):
        for b in range(2):
            dist_out[c * rows : (c + 1) * rows, b * LANES : (b + 1) * LANES] = own[SWEEPS, c, b]

    arcs_told.wait_send()

    @pl.loop(0, SWEEPS)
    def _(sweep):
        for c in range(CHUNKS):
            to_partner(sweep, c).wait_send()
            to_other(sweep, c, own.at[0, c]).wait_send()


def shards(prev_dist, source_node, arc_tail, base_cost, arc_price, capacity, path_arcs, demand):
    arcs = lax.axis_size("arc")
    comms = lax.axis_size("comm")
    rows, span = prev_dist.shape
    vmem = pl.BlockSpec(memory_space=pltpu.VMEM)
    smem = pl.BlockSpec(memory_space=pltpu.SMEM)
    dma = pltpu.SemaphoreType.DMA
    return pl.pallas_call(
        functools.partial(kernel, arcs, comms, arcs * span),
        out_shape=(
            pltpu.VMEM(prev_dist.shape, F32),
            pltpu.VMEM(arc_price.shape, F32),
        ),
        in_specs=[pl.BlockSpec(memory_space=pltpu.HBM)] * 7 + [smem],
        out_specs=(vmem, vmem),
        scratch_shapes=[
            pltpu.VMEM(prev_dist.shape, F32),
            pltpu.VMEM((1, rows), jnp.int32),
            pltpu.VMEM(arc_tail.shape, jnp.int32),
            pltpu.VMEM(arc_price.shape, F32),
            pltpu.VMEM(arc_price.shape, F32),
            pltpu.VMEM(arc_price.shape, F32),
            pltpu.VMEM(path_arcs.shape, jnp.int32),
            dma((7,)),
            pltpu.VMEM((SWEEPS + 1, CHUNKS, 2, rows // CHUNKS, LANES), F32),
            pltpu.VMEM((SWEEPS, CHUNKS, 2, rows // CHUNKS, LANES), F32),
            pltpu.VMEM((SWEEPS, CHUNKS, 2, rows // CHUNKS, LANES), F32),
            pltpu.VMEM((SWEEPS, CHUNKS, 2, rows // CHUNKS, LANES), F32),
            pltpu.VMEM((2, CHUNKS, 2, rows // CHUNKS, LANES), F32),
            pltpu.VMEM((CHUNKS, 2, rows // CHUNKS, LANES), F32),
            pltpu.VMEM((CHUNKS, rows // CHUNKS, 12 * LANES), BF16),
            pltpu.VMEM((2, 8, 12 * LANES, span), HOT),
            pltpu.VMEM((2, 8, 4 * LANES, span), HOT),
            pltpu.VMEM((2, 8, span), jnp.int32),
            pltpu.VMEM((3, 2, 8, span), F32),
            pltpu.VMEM((2, 2, 8, span), F32),
            pltpu.VMEM((2, 2, 8, span), F32),
            pltpu.VMEM((8, LANES), F32),
            pltpu.VMEM((arcs, 8, LANES), F32),
            pltpu.VMEM((LANES, 32 * LANES), HOT),
            pltpu.VMEM((64, 32 * LANES), BF16),
            pltpu.VMEM((16, span), F32),
            pltpu.VMEM((comms, 16, span), F32),
            pltpu.VMEM((8, LANES), F32),
            pltpu.VMEM((ROW, 8, LANES), F32),
            pltpu.VMEM((8, LANES), F32),
            pltpu.VMEM((arcs // ROW, 8, LANES), F32),
            dma((2, SWEEPS, CHUNKS)),
            dma((2, SWEEPS, CHUNKS)),
            dma,
            dma,
            dma((2, ROW)),
            dma((2, ROW)),
            dma((2, arcs // ROW)),
            dma((2, arcs // ROW)),
            dma((7,)),
            dma((7,)),
        ],
        compiler_params=pltpu.CompilerParams(
            collective_id=0, has_side_effects=True, vmem_limit_bytes=63 * 1024 * 1024 - 65536
        ),
    )(
        prev_dist, source_node.reshape(1, rows), arc_tail, base_cost, arc_price, capacity,
        path_arcs, demand,
    )


def solution(mesh):
    in_specs = (
        P("comm", "arc"),
        P("comm"),
        P(None, "arc"),
        P(None, "arc"),
        P(None, "arc"),
        P(None, "arc"),
        P(("comm", "arc"), None),
        P(("comm", "arc")),
    )
    out_specs = (P("comm", "arc"), P(None, "arc"))
    return jax.shard_map(shards, mesh=mesh, in_specs=in_specs, out_specs=out_specs, check_vma=False)
```
